32 devices in a mesh: gx: 4 (over x, core), gy: 4 (over z), gz: 2 (over y).
Axes of the slice: x: 2, y: 2, z: 4, core: 2. Of those that a mesh axis runs over, the one named last changes fastest.
Arguments:
- field: float32 [64, 1024, 256], P('gx', 'gy', 'gz'), may hold values from -6 to 6
- source: float32 [64, 1024, 256], P('gx', 'gy', 'gz'), may hold values from -6 to 6
Outputs:
- smoothed: float32 [64, 1024, 256], P('gx', 'gy', 'gz')
The draws below stay inside these ranges and needn't reach their ends.
All inputs are finite; a program needn't handle non-finite values.
Results may differ from the reference program's by a relative error of at most 0.00002.
Values sent between devices are 32-bit elements; how exact they have to be, the bound alone decides.
A program may use at most 64 MiB of HBM per device.

```python
import jax
import jax.numpy as jnp

SWEEPS = 3
NX = 64
NY = 1024
NZ = 256


def block_levels(key, shape, split, least, top_value):
    def one(position, parts):
        draws = jax.random.uniform(jax.random.fold_in(jax.random.fold_in(key, 6), position), (parts,), jnp.float32, least / len(split), top_value / len(split))
        return jnp.repeat(jnp.exp(draws), shape[position] // parts).reshape((-1,) + (1,) * (len(shape) - position - 1))

    loudness = one(*split[0])
    for cut in split[1:]:
        loudness = loudness * one(*cut)
    return loudness


def bell_draw(own_key, shape, spread, most, shards=(), held_as=jnp.bfloat16):
    entries = jax.random.normal(own_key, shape, jnp.float32) * spread
    if len(shards) > 0:
        entries = block_levels(own_key, shape, shards, -0.22, 0.18) * entries
    return jnp.clip(entries, min=-most, max=most).astype(held_as)


def setup_inputs(seed: int = 0) -> dict:
    key_of = jax.random.split(jax.random.key(seed), 3)
    field = bell_draw(key_of[0], (NX, NY, NZ), 1.0, 6.0, ((0, 4), (1, 4), (2, 2)), jnp.float32)
    source = bell_draw(key_of[1], (NX, NY, NZ), 1.0, 6.0, ((0, 4), (1, 4), (2, 2)), jnp.float32)
    return dict(field=field, source=source)


def relax(values, source, parity, colour):
    padded = jnp.pad(values, ((1, 1), (0, 0), (0, 0)))
    beside = padded[2:] + padded[:-2]
    beside = beside + jnp.roll(values, -1, 1) + jnp.roll(values, 1, 1)
    beside = beside + jnp.roll(values, -1, 2) + jnp.roll(values, 1, 2)
    return jnp.where(parity == colour, (source + beside) / 6.0, values)


def reference(field, source):
    nx, ny, nz = field.shape
    parity = (jnp.arange(nx, dtype=jnp.int32)[:, None, None] + jnp.arange(ny, dtype=jnp.int32)[None, :, None] + jnp.arange(nz, dtype=jnp.int32)[None, None, :]) % 2
    values = field
    for sweep in range(SWEEPS):
        values = relax(values, source, parity, 0)
        values = relax(values, source, parity, 1)
    return values
```

```python
import functools

import jax
import jax.numpy as jnp
from jax import lax
from jax.experimental import pallas as pl
from jax.experimental.pallas import tpu as pltpu
from jax.sharding import PartitionSpec as P

SWEEPS = 3
MESH = pl.DeviceIdType.MESH
PAD = 16
X, Y, Z, XY, YZ, XZ, SX, SY, SZ = 0, 2, 4, 6, 10, 14, 18, 20, 22
SIXTH = 1.0 / 6.0


def kernel(
    sizes, f_hbm, s_hbm, ov, fv, sv, x, src, eb, er, qb, sq, yzb, sqs,
    pk, jb, yzs, sys_, xg, jr, zr, xyr, yzr, xzr, syr, szr, send, recv, fsem, ssem,
):
    ngx, ngy, ngz = sizes
    planes, rows, cols = f_hbm.shape
    nm = planes // 2
    ng = rows // 8
    gx, gy, gz = (lax.axis_index(a) for a in ("gx", "gy", "gz"))
    has = (gx > 0, gx < ngx - 1)
    nz = 1 if ngz == 2 else 2
    y_to = (lax.rem(gy + ngy - 1, ngy), lax.rem(gy + 1, ngy))
    z_to = (lax.rem(gz + 1, ngz), lax.rem(gz + ngz - 1, ngz))[:nz]
    x_to = (gx - 1, gx + 1)
    last = cols - 1

    def load(ref, to, sem, m):
        return pltpu.make_async_copy(ref.at[pl.ds(2 * m, 2)], to.at[pl.ds(2 * m, 2)], sem.at[m])

    order = [m for a in range(nm // 2) for m in (a, nm - 1 - a)]
    for m in order:
        load(f_hbm, fv, fsem, m).start()
    for m in order:
        load(s_hbm, sv, ssem, m).start()

    barrier = pltpu.get_barrier_semaphore()

    def greet(device):
        pl.semaphore_signal(barrier, inc=1, device_id=device, device_id_type=MESH)

    for y in y_to:
        greet({"gy": y})
        for z in z_to:
            greet({"gy": y, "gz": z})
    for z in z_to:
        greet({"gz": z})
    for sx in range(2):

        @pl.when(has[sx])
        def _():
            greet({"gx": x_to[sx]})
            for y in y_to:
                greet({"gx": x_to[sx], "gy": y})
            for z in z_to:
                greet({"gx": x_to[sx], "gz": z})

    sub = lax.broadcasted_iota(jnp.int32, (8, cols), 0)
    lane = lax.broadcasted_iota(jnp.int32, (8, cols), 1)
    odd = lax.rem(sub + lane, 2) == 1
    first, final_lane = lane == 0, lane == last
    quad = lax.div(lane, 4)
    pos = lax.rem(lane, 4)
    pos0, pos1, pos3, low_half = pos == 0, pos == 1, pos == 3, pos < 2
    odd_q = lax.rem(sub + jnp.where(pos1, 1, 0), 2) == 1
    top, bottom = sub == 0, sub == 7
    hi_quad = ng % (cols // 4)
    in_lo, in_hi = quad == cols // 4 - 1, quad == hi_quad
    zero = jnp.zeros((8, cols), jnp.float32)

    def roll(v, by):
        by = by % cols
        return v if by == 0 else pltpu.roll(v, by, 1)

    for sx in range(2):
        m = (0, nm + 1)[sx]

        @pl.when(jnp.logical_not(has[sx]))
        def _():
            for c in range(2):
                x[c, m] = jnp.zeros((rows + 2 * PAD, cols), jnp.float32)
            eb[m] = zero
            qb[m] = zero

    def copy(src_ref, dst_ref, device, slot, t):
        return pltpu.make_async_remote_copy(
            src_ref=src_ref, dst_ref=dst_ref, send_sem=send.at[slot, t], recv_sem=recv.at[slot, t],
            device_id=device, device_id_type=MESH,
        )

    edge_m = (0, nm - 1)

    def msg_x(sx, t):
        return copy(x.at[1, edge_m[sx] + 1, pl.ds(PAD, rows)], xg.at[1 - sx, t], {"gx": x_to[sx]}, X + sx, t)

    def msg_y(sy, t):
        return copy(jb.at[sy, t], jr.at[1 - sy, t], {"gy": y_to[sy]}, Y + sy, t)

    def msg_z(zd, t):
        return copy(pk.at[t], zr.at[zd, t], {"gz": z_to[zd]}, Z + zd, t)

    def msg_xy(sx, sy, t):
        return copy(
            jb.at[sy, t, edge_m[sx]], xyr.at[1 - sx, 1 - sy, t], {"gx": x_to[sx], "gy": y_to[sy]}, XY + 2 * sx + sy, t
        )

    def msg_yz(sy, zd, t):
        return copy(yzs.at[sy, t], yzr.at[1 - sy, zd, t], {"gy": y_to[sy], "gz": z_to[zd]}, YZ + 2 * sy + zd, t)

    def msg_xz(sx, zd, t):
        return copy(
            pk.at[t, edge_m[sx]], xzr.at[1 - sx, zd, t], {"gx": x_to[sx], "gz": z_to[zd]}, XZ + 2 * sx + zd, t
        )

    def msg_sx(sx):
        return copy(
            src.at[0, edge_m[sx] + 1, pl.ds(PAD, rows)], src.at[0, (nm + 1, 0)[sx], pl.ds(PAD, rows)],
            {"gx": x_to[sx]}, SX + sx, 0,
        )

    def msg_sy(sy):
        return copy(sys_.at[sy], syr.at[1 - sy], {"gy": y_to[sy]}, SY + sy, 0)

    def msg_sz(zd):
        return copy(sqs, szr.at[zd], {"gz": z_to[zd]}, SZ + zd, 0)

    def send_far(t):
        for sy in range(2):
            for zd in range(nz):
                msg_yz(sy, zd, t).start()
        for sx in range(2):

            @pl.when(has[sx])
            def _():
                for sy in range(2):
                    msg_xy(sx, sy, t).start()

        for sy in range(2):
            msg_y(sy, t).start()

    def send_x(t):
        for sx in range(2):

            @pl.when(has[sx])
            def _():
                for zd in range(nz):
                    msg_xz(sx, zd, t).start()
                msg_x(sx, t).start()

    def send_z(t):
        for zd in range(nz):
            msg_z(zd, t).start()

    def rows_of(g, shift=0):
        return pl.ds(PAD + 8 * g + shift, 8)

    def keep_rows(t, m, g, y, sy):
        if sy == 0:
            jb[0, t, m] = y[0:2]
            yzs[0, t, pl.ds(m, 1), :] = roll(y, 4 * hi_quad + 2)[0:1]
        else:
            jb[1, t, m] = y[6:8]
            yzs[1, t, pl.ds(m, 1), :] = roll(y, -2)[7:8]

    def packed(acc, g, y):
        return jnp.where(quad == g, roll(y, 4 * g + 2), acc)

    def field_plane(m, carry):
        load(f_hbm, fv, fsem, m).wait()
        acc = [zero] * 4
        for g in range(ng):
            rs = pl.ds(8 * g, 8)
            y = jnp.where(odd, fv[2 * m, rs, :], fv[2 * m + 1, rs, :])
            x[1, m + 1, rows_of(g), :] = y
            acc[g % 4] = packed(acc[g % 4], g, y)
            if g == 0:
                keep_rows(0, m, g, y, 0)
            if g == ng - 1:
                keep_rows(0, m, g, y, 1)
        pk[0, m] = (acc[0] + acc[1]) + (acc[2] + acc[3])
        return carry

    def source_plane(m, carry):
        load(s_hbm, sv, ssem, m).wait()
        acc = [zero] * 4
        for g in range(ng):
            rs = pl.ds(8 * g, 8)
            low, high = sv[2 * m, rs, :], sv[2 * m + 1, rs, :]
            red = jnp.where(odd, high, low)
            src[0, m + 1, rows_of(g), :] = red
            src[1, m + 1, rows_of(g), :] = jnp.where(odd, low, high)
            acc[g % 4] = packed(acc[g % 4], g, red)
            if g == 0:
                sys_[0, pl.ds(m, 1), :] = red[0:1]
            if g == ng - 1:
                sys_[1, pl.ds(m, 1), :] = red[7:8]
        sqs[m] = (acc[0] + acc[1]) + (acc[2] + acc[3])
        return carry

    lax.fori_loop(0, nm, field_plane, 0)
    near = [h.astype(jnp.int32) for h in has]
    pl.semaphore_wait(barrier, 2 + 3 * nz + (near[0] + near[1]) * (3 + nz))
    send_far(0)
    send_x(0)
    send_z(0)
    lax.fori_loop(0, nm, source_plane, 0)
    for sy in range(2):
        msg_sy(sy).start()
    for zd in range(nz):
        msg_sz(zd).start()
    for sx in range(2):

        @pl.when(has[sx])
        def _():
            msg_sx(sx).start()

    def tile(c, m, g, edge, side=None):
        d = 1 - c
        rs = rows_of(g)
        here = x[d, m + 1, rs, :]
        if side is None:
            below, above = x[d, m, rs, :], x[d, m + 2, rs, :]
            beside = jnp.where(odd, above, below) if c == 0 else jnp.where(odd, below, above)
        else:
            beside = x[d, m + 1 + side, rs, :]
        total = (src[c, m + 1, rs, :] + here) + (beside + x[d, m + 1, rows_of(g, -1), :])
        total = total + x[d, m + 1, rows_of(g, 1), :]
        total = total + jnp.where(first, edge, roll(here, 1))
        total = total + jnp.where(final_lane, edge, roll(here, -1))
        return total * jnp.float32(SIXTH)

    def edge_at(v, g):
        return roll(v, -(4 * g + 2))

    def red_plane(m, groups, side=None):
        v = eb[m + 1]
        for g in groups:
            x[0, m + 1, rows_of(g), :] = tile(0, m, g, edge_at(v, g), side)

    def put(m, g, y, final):
        if final:
            red = x[0, m + 1, rows_of(g), :]
            rs = pl.ds(8 * g, 8)
            ov[2 * m, rs, :] = jnp.where(odd, y, red)
            ov[2 * m + 1, rs, :] = jnp.where(odd, red, y)
        else:
            x[1, m + 1, rows_of(g), :] = y

    def black_plane(m, groups, t, final):
        v = er[m]
        acc = [zero] * 4
        for g in groups:
            y = tile(1, m, g, edge_at(v, g))
            put(m, g, y, final)
            if not final:
                acc[g % 4] = packed(acc[g % 4], g, y)
        if not final:
            pk[t + 1, m] = pk[t + 1, m] + ((acc[0] + acc[1]) + (acc[2] + acc[3]))

    inner = range(1, ng - 1)

    def swapped(lo, hi):
        return jnp.where(pos1, roll(hi, -1), roll(lo, 1))

    for t in range(SWEEPS):
        final = t == SWEEPS - 1
        hi_z = nz - 1
        for zd in range(nz):
            msg_z(zd, t).wait_recv()
        for m in range(nm):
            lo, hi = zr[0, t, m], zr[hi_z, t, m]
            qb[m + 1] = jnp.where(low_half, lo, hi)
            eb[m + 1] = swapped(lo, hi)
        if t == 0:
            pass

        def red_inner(m, carry):
            red_plane(m, inner)
            return carry

        lax.fori_loop(1, nm - 1, red_inner, 0)

        for sx in range(2):
            m, at = ((-1, 0), (nm, nm + 1))[sx]

            @pl.when(has[sx])
            def _():
                for zd in range(nz):
                    msg_xz(1 - sx, zd, t).wait_recv()
                lo, hi = xzr[sx, 0, t], xzr[sx, hi_z, t]
                qb[at] = jnp.where(low_half, lo, hi)
                eb[at] = swapped(lo, hi)
                msg_x(1 - sx, t).wait_recv()
                if t == 0:
                    msg_sx(1 - sx).wait_recv()
                x[1, at, pl.ds(PAD, rows), :] = xg[sx, t]
                red_plane(m, inner, (1, -1)[sx])

        for m in edge_m:
            red_plane(m, inner)

        if t == 0:
            for zd in range(nz):
                msg_sz(zd).wait_recv()
            for m in range(nm):
                sq[m] = jnp.where(low_half, szr[0, m], szr[hi_z, m])
            for sy in range(2):
                msg_sy(sy).wait_recv()
                for m in range(nm):
                    src[0, m + 1, pl.ds((PAD + rows, PAD - 1)[sy], 1), :] = syr[1 - sy, pl.ds(m, 1), :]
        for sy in range(2):
            msg_y(sy, t).wait_recv()
            for m in range(nm):
                x[1, m + 1, pl.ds((PAD + rows, PAD - 2)[sy], 2), :] = jr[1 - sy, t, m]
        for sx in range(2):

            @pl.when(has[sx])
            def _():
                for sy in range(2):
                    msg_xy(1 - sx, sy, t).wait_recv()
                    x[1, (0, nm + 1)[sx], pl.ds((PAD + rows, PAD - 2)[sy], 2), :] = xyr[sx, 1 - sy, t]

        low8 = lax.rem(lax.broadcasted_iota(jnp.int32, (nm, cols), 1), 4)
        for sy in range(2):
            for zd in range(nz):
                msg_yz(sy, zd, t).wait_recv()
            lo, hi = yzr[1 - sy, 0, t], yzr[1 - sy, hi_z, t]
            yzb[1 - sy] = jnp.where(low8 < 2, lo, hi)
            yzb[2 + 1 - sy] = jnp.where(low8 == 1, pltpu.roll(hi, last, 1), pltpu.roll(lo, 1, 1))

        def spread(k, m):
            return jnp.broadcast_to(yzb[k, pl.ds(m, 1), :], (8, cols))

        for sx in range(2):
            m = (-1, nm)[sx]

            @pl.when(has[sx])
            def _():
                red_plane(m, (0, ng - 1), (1, -1)[sx])

        for m in range(nm):
            red_plane(m, (0, ng - 1))
            for g, k in ((-1, 2), (ng, 3)):
                x[0, m + 1, rows_of(g), :] = tile(0, m, g, edge_at(spread(k, m), g))
            own, q = pk[t, m], qb[m + 1]
            zsum = roll(jnp.where(pos0, q, own), 1) + roll(jnp.where(pos3, q, own), -1)
            beside = jnp.where(odd_q, qb[m + 2], qb[m])
            up = jnp.where(bottom, roll(jnp.where(in_lo, spread(0, m), q), 4), q)
            down = jnp.where(top, roll(jnp.where(in_hi, spread(1, m), q), -4), q)
            total = (sq[m] + q) + (beside + pltpu.roll(up, 1, 0)) + (pltpu.roll(down, 7, 0) + zsum)
            red = total * jnp.float32(SIXTH)
            er[m] = swapped(red, red)

        if not final:
            for sx in range(2):

                @pl.when(has[sx])
                def _():
                    msg_x(sx, t).wait_send()

        for m in range(nm):
            v = er[m]
            acc = zero
            for sy, g in ((0, 0), (1, ng - 1)):
                y = tile(1, m, g, edge_at(v, g))
                put(m, g, y, final)
                if not final:
                    keep_rows(t + 1, m, g, y, sy)
                    acc = packed(acc, g, y)
            if not final:
                pk[t + 1, m] = acc
        if not final:
            send_far(t + 1)
        for m in edge_m:
            black_plane(m, inner, t, final)
        if not final:
            send_x(t + 1)

        def black_inner(m, carry):
            black_plane(m, inner, t, final)
            return carry

        lax.fori_loop(1, nm - 1, black_inner, 0)
        if not final:
            send_z(t + 1)

    for sy in range(2):
        msg_sy(sy).wait_send()
    for zd in range(nz):
        msg_sz(zd).wait_send()
    for t in range(SWEEPS):
        for sy in range(2):
            msg_y(sy, t).wait_send()
            for zd in range(nz):
                msg_yz(sy, zd, t).wait_send()
        for zd in range(nz):
            msg_z(zd, t).wait_send()
    for sx in range(2):

        @pl.when(has[sx])
        def _():
            msg_sx(sx).wait_send()
            msg_x(sx, SWEEPS - 1).wait_send()
            for t in range(SWEEPS):
                for sy in range(2):
                    msg_xy(sx, sy, t).wait_send()
                for zd in range(nz):
                    msg_xz(sx, zd, t).wait_send()


def solution(mesh):
    sizes = tuple(mesh.shape[a] for a in ("gx", "gy", "gz"))

    def on_device(field, source):
        planes, rows, cols = field.shape
        nm, ng, nz = planes // 2, rows // 8, 1 if sizes[2] == 2 else 2
        assert planes % 4 == 0 and nm >= 4 and rows % 8 == 0 and cols == 128 and 4 * ng <= cols
        f32 = jnp.float32
        vm = lambda *shape: pltpu.VMEM(shape, f32)
        return pl.pallas_call(
            functools.partial(kernel, sizes),
            out_shape=jax.ShapeDtypeStruct(field.shape, f32),
            in_specs=[pl.BlockSpec(memory_space=pltpu.HBM)] * 2,
            out_specs=pl.BlockSpec(memory_space=pltpu.VMEM),
            scratch_shapes=[
                vm(*field.shape),
                vm(*field.shape),
                vm(2, nm + 2, rows + 2 * PAD, cols),
                vm(2, nm + 2, rows + 2 * PAD, cols),
                vm(nm + 2, 8, cols),
                vm(nm, 8, cols),
                vm(nm + 2, 8, cols),
                vm(nm, 8, cols),
                vm(4, nm, cols),
                vm(nm, 8, cols),
                vm(SWEEPS, nm, 8, cols),
                vm(2, SWEEPS, nm, 2, cols),
                vm(2, SWEEPS, nm, cols),
                vm(2, nm, cols),
                vm(2, SWEEPS, rows, cols),
                vm(2, SWEEPS, nm, 2, cols),
                vm(nz, SWEEPS, nm, 8, cols),
                vm(2, 2, SWEEPS, 2, cols),
                vm(2, nz, SWEEPS, nm, cols),
                vm(2, nz, SWEEPS, 8, cols),
                vm(2, nm, cols),
                vm(nz, nm, 8, cols),
                pltpu.SemaphoreType.DMA((24, SWEEPS)),
                pltpu.SemaphoreType.DMA((24, SWEEPS)),
                pltpu.SemaphoreType.DMA((nm,)),
                pltpu.SemaphoreType.DMA((nm,)),
            ],
            compiler_params=pltpu.CompilerParams(
                collective_id=0, has_side_effects=True, vmem_limit_bytes=50 * 1024 * 1024
            ),
        )(field, source)

    spec = P("gx", "gy", "gz")
    return jax.shard_map(on_device, mesh=mesh, in_specs=(spec, spec), out_specs=spec, check_vma=False)
```

```python
import functools

import jax
import jax.numpy as jnp
from jax import lax
from jax.experimental import pallas as pl
from jax.experimental.pallas import tpu as pltpu
from jax.sharding import PartitionSpec as P

SWEEPS = 3
MESH = pl.DeviceIdType.MESH
PAD = 16
X, Y, Z, XY, YZ, XZ, SX, SY, SZ = 0, 2, 4, 6, 10, 14, 18, 20, 22
SIXTH = 1.0 / 6.0


def kernel(
    sizes, f_hbm, s_hbm, ov, fv, sv, x0, x1, s0, s1, eb, er, qb, sq, yzb, sqs,
    pk, jb, yzs, sys_, xg, jr, zr, xyr, yzr, xzr, syr, szr, send, recv, fsem, ssem,
):
    ngx, ngy, ngz = sizes
    planes, rows, cols = f_hbm.shape
    nm = planes // 2
    ng = rows // 8
    gx, gy, gz = (lax.axis_index(a) for a in ("gx", "gy", "gz"))
    has = (gx > 0, gx < ngx - 1)
    nz = 1 if ngz == 2 else 2
    y_to = (lax.rem(gy + ngy - 1, ngy), lax.rem(gy + 1, ngy))
    z_to = (lax.rem(gz + 1, ngz), lax.rem(gz + ngz - 1, ngz))[:nz]
    x_to = (gx - 1, gx + 1)
    last = cols - 1
    edge_m = (0, nm - 1)

    def load(ref, to, sem, m):
        return pltpu.make_async_copy(ref.at[pl.ds(2 * m, 2)], to.at[pl.ds(2 * m, 2)], sem.at[m])

    def load_ends(sy):
        rs = pl.ds((0, rows - 8)[sy], 8)
        return pltpu.make_async_copy(f_hbm.at[:, rs], fv.at[:, rs], fsem.at[nm + sy])

    def load_field(m):
        at = (pl.ds(2 * m, 2), pl.ds(8, rows - 16))
        return pltpu.make_async_copy(f_hbm.at[at], fv.at[at], fsem.at[m])

    order = [*edge_m, *range(1, nm - 1)]
    for sy in range(2):
        load_ends(sy).start()
    for m in order:
        load_field(m).start()
    for m in order:
        load(s_hbm, sv, ssem, m).start()

    barrier = pltpu.get_barrier_semaphore()

    def greet(device):
        pl.semaphore_signal(barrier, inc=1, device_id=device, device_id_type=MESH)

    for y in y_to:
        greet({"gy": y})
        for z in z_to:
            greet({"gy": y, "gz": z})
    for z in z_to:
        greet({"gz": z})
    for sx in range(2):

        @pl.when(has[sx])
        def _():
            greet({"gx": x_to[sx]})
            for y in y_to:
                greet({"gx": x_to[sx], "gy": y})
            for z in z_to:
                greet({"gx": x_to[sx], "gz": z})

    sub = lax.broadcasted_iota(jnp.int32, (8, cols), 0)
    lane = lax.broadcasted_iota(jnp.int32, (8, cols), 1)
    odd = lax.rem(sub + lane, 2) == 1
    first, final_lane = lane == 0, lane == last
    quad = lax.div(lane, 4)
    pos = lax.rem(lane, 4)
    pos0, pos1, pos3, low_half = pos == 0, pos == 1, pos == 3, pos < 2
    odd_q = lax.rem(sub + jnp.where(pos1, 1, 0), 2) == 1
    top, bottom = sub == 0, sub == 7
    hi_quad = ng % (cols // 4)
    in_lo, in_hi = quad == cols // 4 - 1, quad == hi_quad
    zero = jnp.zeros((8, cols), jnp.float32)

    def roll(v, by):
        by = by % cols
        return v if by == 0 else pltpu.roll(v, by, 1)

    for sx in range(2):
        m = (0, nm + 1)[sx]

        @pl.when(jnp.logical_not(has[sx]))
        def _():
            for c in range(2):
                (x0, x1)[c][m] = jnp.zeros((rows + 2 * PAD, cols), jnp.float32)
            eb[m] = zero
            qb[m] = zero

    def copy(src_ref, dst_ref, device, slot, t):
        return pltpu.make_async_remote_copy(
            src_ref=src_ref, dst_ref=dst_ref, send_sem=send.at[slot, t], recv_sem=recv.at[slot, t],
            device_id=device, device_id_type=MESH,
        )


    def msg_x(sx, t):
        return copy(x1.at[edge_m[sx] + 1, pl.ds(PAD, rows)], xg.at[1 - sx, t], {"gx": x_to[sx]}, X + sx, t)

    def msg_y(sy, t):
        return copy(jb.at[sy, t], jr.at[1 - sy, t], {"gy": y_to[sy]}, Y + sy, t)

    def msg_z(zd, t):
        return copy(pk.at[t], zr.at[zd, t], {"gz": z_to[zd]}, Z + zd, t)

    def msg_xy(sx, sy, t):
        return copy(
            jb.at[sy, t, edge_m[sx]], xyr.at[1 - sx, 1 - sy, t], {"gx": x_to[sx], "gy": y_to[sy]}, XY + 2 * sx + sy, t
        )

    def msg_yz(sy, zd, t):
        return copy(yzs.at[sy, t], yzr.at[1 - sy, zd, t], {"gy": y_to[sy], "gz": z_to[zd]}, YZ + 2 * sy + zd, t)

    def msg_xz(sx, zd, t):
        return copy(
            pk.at[t, edge_m[sx]], xzr.at[1 - sx, zd, t], {"gx": x_to[sx], "gz": z_to[zd]}, XZ + 2 * sx + zd, t
        )

    def msg_sx(sx):
        return copy(
            s0.at[edge_m[sx] + 1, pl.ds(PAD, rows)], s0.at[(nm + 1, 0)[sx], pl.ds(PAD, rows)],
            {"gx": x_to[sx]}, SX + sx, 0,
        )

    def msg_sy(sy):
        return copy(sys_.at[sy], syr.at[1 - sy], {"gy": y_to[sy]}, SY + sy, 0)

    def msg_sz(zd):
        return copy(sqs, szr.at[zd], {"gz": z_to[zd]}, SZ + zd, 0)

    def send_far(t):
        for sy in range(2):
            for zd in range(nz):
                msg_yz(sy, zd, t).start()
        for sx in range(2):

            @pl.when(has[sx])
            def _():
                for sy in range(2):
                    msg_xy(sx, sy, t).start()

        for sy in range(2):
            msg_y(sy, t).start()

    def send_x(t):
        for sx in range(2):

            @pl.when(has[sx])
            def _():
                msg_x(sx, t).start()

    def send_z(t):
        for sx in range(2):

            @pl.when(has[sx])
            def _():
                for zd in range(nz):
                    msg_xz(sx, zd, t).start()

        for zd in range(nz):
            msg_z(zd, t).start()

    def rows_of(g, shift=0):
        return pl.ds(PAD + 8 * g + shift, 8)

    def keep_rows(t, m, g, y, sy):
        if sy == 0:
            jb[0, t, m] = y[0:2]
            yzs[0, t, pl.ds(m, 1), :] = roll(y, 4 * hi_quad + 2)[0:1]
        else:
            jb[1, t, m] = y[6:8]
            yzs[1, t, pl.ds(m, 1), :] = roll(y, -2)[7:8]

    def packed(acc, g, y):
        return jnp.where(quad == g, roll(y, 4 * g + 2), acc)

    def field_rows(m, groups):
        for g in groups:
            rs = pl.ds(8 * g, 8)
            x1[m + 1, rows_of(g), :] = jnp.where(odd, fv[2 * m, rs, :], fv[2 * m + 1, rs, :])

    def field_plane(m, carry):
        load_field(m).wait()
        field_rows(m, inner)
        return carry

    def several(lo, hi, n, body):
        n = max(k for k in range(1, n + 1) if (hi - lo) % k == 0)

        def step(i, carry):
            for k in range(n):
                body(lo + n * i + k)
            return carry

        lax.fori_loop(0, (hi - lo) // n, step, 0)

    def pack_plane(t, m):
        acc = [zero] * 4
        for g in range(ng):
            acc[g % 4] = packed(acc[g % 4], g, x1[m + 1, rows_of(g), :])
        pk[t, m] = (acc[0] + acc[1]) + (acc[2] + acc[3])

    def pack(t):
        several(0, nm, 4, functools.partial(pack_plane, t))

    inner = range(1, ng - 1)

    def source_plane(m, carry):
        load(s_hbm, sv, ssem, m).wait()
        acc = [zero] * 4
        for g in range(ng):
            rs = pl.ds(8 * g, 8)
            low, high = sv[2 * m, rs, :], sv[2 * m + 1, rs, :]
            red = jnp.where(odd, high, low)
            s0[m + 1, rows_of(g), :] = red
            s1[m, rows_of(g), :] = jnp.where(odd, low, high)
            acc[g % 4] = packed(acc[g % 4], g, red)
            if g == 0:
                sys_[0, pl.ds(m, 1), :] = red[0:1]
            if g == ng - 1:
                sys_[1, pl.ds(m, 1), :] = red[7:8]
        sqs[m] = (acc[0] + acc[1]) + (acc[2] + acc[3])
        return carry

    with jax.named_scope("ends"):
        for sy, g in ((0, 0), (1, ng - 1)):
            load_ends(sy).wait()
            for m in range(nm):
                field_rows(m, (g,))
                keep_rows(0, m, g, x1[m + 1, rows_of(g), :], sy)
    near = [h.astype(jnp.int32) for h in has]
    with jax.named_scope("barrier"):
        pl.semaphore_wait(barrier, 2 + 3 * nz + (near[0] + near[1]) * (3 + nz))
    send_far(0)
    with jax.named_scope("field"):
        for m in edge_m:
            field_plane(m, 0)
        send_x(0)
        lax.fori_loop(1, nm - 1, field_plane, 0)
    with jax.named_scope("pack"):
        pack(0)
    send_z(0)
    with jax.named_scope("source"):
        lax.fori_loop(0, nm, source_plane, 0)
    for sy in range(2):
        msg_sy(sy).start()
    for zd in range(nz):
        msg_sz(zd).start()
    for sx in range(2):

        @pl.when(has[sx])
        def _():
            msg_sx(sx).start()

    def tile(c, m, g, edge, side=None):
        v = (x1, x0)[c]
        rs = rows_of(g)
        here = v[m + 1, rs, :]
        if side is None:
            below, above = v[m, rs, :], v[m + 2, rs, :]
            beside = jnp.where(odd, above, below) if c == 0 else jnp.where(odd, below, above)
        else:
            beside = v[m + 1 + side, rs, :]
        given = s0[m + 1, rs, :] if c == 0 else s1[m, rs, :]
        total = (given + here) + (beside + v[m + 1, rows_of(g, -1), :])
        total = total + v[m + 1, rows_of(g, 1), :]
        total = total + jnp.where(first, edge, roll(here, 1))
        total = total + jnp.where(final_lane, edge, roll(here, -1))
        return total * jnp.float32(SIXTH)

    def edge_at(v, g):
        return roll(v, -(4 * g + 2))

    def red_plane(m, groups, side=None):
        v = eb[m + 1]
        for g in groups:
            x0[m + 1, rows_of(g), :] = tile(0, m, g, edge_at(v, g), side)

    def put(m, g, y, final):
        if final:
            red = x0[m + 1, rows_of(g), :]
            rs = pl.ds(8 * g, 8)
            ov[2 * m, rs, :] = jnp.where(odd, y, red)
            ov[2 * m + 1, rs, :] = jnp.where(odd, red, y)
        else:
            x1[m + 1, rows_of(g), :] = y

    def black_plane(m, groups, final):
        v = er[m]
        for g in groups:
            put(m, g, tile(1, m, g, edge_at(v, g)), final)

    def swapped(lo, hi):
        return jnp.where(pos1, roll(hi, -1), roll(lo, 1))

    for t in range(SWEEPS):
        final = t == SWEEPS - 1
        hi_z = nz - 1
        with jax.named_scope("waitz"):
            for zd in range(nz):
                msg_z(zd, t).wait_recv()
        for m in range(nm):
            lo, hi = zr[0, t, m], zr[hi_z, t, m]
            qb[m + 1] = jnp.where(low_half, lo, hi)
            eb[m + 1] = swapped(lo, hi)
        with jax.named_scope("P1"):
            several(1, nm - 1, 3, lambda m: red_plane(m, inner))

        with jax.named_scope("P2x"):
            for sx in range(2):
                m, at = ((-1, 0), (nm, nm + 1))[sx]

                @pl.when(has[sx])
                def _():
                    for zd in range(nz):
                        msg_xz(1 - sx, zd, t).wait_recv()
                    lo, hi = xzr[sx, 0, t], xzr[sx, hi_z, t]
                    qb[at] = jnp.where(low_half, lo, hi)
                    eb[at] = swapped(lo, hi)
                    msg_x(1 - sx, t).wait_recv()
                    if t == 0:
                        msg_sx(1 - sx).wait_recv()
                    x1[at, pl.ds(PAD, rows), :] = xg[sx, t]
                    red_plane(m, inner, (1, -1)[sx])

        with jax.named_scope("P2e"):
            for m in edge_m:
                red_plane(m, inner)

        with jax.named_scope("P3wait"):
            if t == 0:
                for zd in range(nz):
                    msg_sz(zd).wait_recv()
                for m in range(nm):
                    sq[m] = jnp.where(low_half, szr[0, m], szr[hi_z, m])
                for sy in range(2):
                    msg_sy(sy).wait_recv()
                    for m in range(nm):
                        s0[m + 1, pl.ds((PAD + rows, PAD - 1)[sy], 1), :] = syr[1 - sy, pl.ds(m, 1), :]
            for sy in range(2):
                msg_y(sy, t).wait_recv()
                for m in range(nm):
                    x1[m + 1, pl.ds((PAD + rows, PAD - 2)[sy], 2), :] = jr[1 - sy, t, m]
            for sx in range(2):

                @pl.when(has[sx])
                def _():
                    for sy in range(2):
                        msg_xy(1 - sx, sy, t).wait_recv()
                        x1[(0, nm + 1)[sx], pl.ds((PAD + rows, PAD - 2)[sy], 2), :] = xyr[sx, 1 - sy, t]

            low8 = lax.rem(lax.broadcasted_iota(jnp.int32, (nm, cols), 1), 4)
            for sy in range(2):
                for zd in range(nz):
                    msg_yz(sy, zd, t).wait_recv()
                lo, hi = yzr[1 - sy, 0, t], yzr[1 - sy, hi_z, t]
                yzb[1 - sy] = jnp.where(low8 < 2, lo, hi)
                yzb[2 + 1 - sy] = jnp.where(low8 == 1, pltpu.roll(hi, last, 1), pltpu.roll(lo, 1, 1))

        def spread(k, m):
            return jnp.broadcast_to(yzb[k, pl.ds(m, 1), :], (8, cols))

        with jax.named_scope("P3red"):
            for sx in range(2):
                m = (-1, nm)[sx]

                @pl.when(has[sx])
                def _():
                    red_plane(m, (0, ng - 1), (1, -1)[sx])

            for m in range(nm):
                red_plane(m, (0, ng - 1))
                for g, k in ((-1, 2), (ng, 3)):
                    x0[m + 1, rows_of(g), :] = tile(0, m, g, edge_at(spread(k, m), g))
                own, q = pk[t, m], qb[m + 1]
                zsum = roll(jnp.where(pos0, q, own), 1) + roll(jnp.where(pos3, q, own), -1)
                beside = jnp.where(odd_q, qb[m + 2], qb[m])
                up = jnp.where(bottom, roll(jnp.where(in_lo, spread(0, m), q), 4), q)
                down = jnp.where(top, roll(jnp.where(in_hi, spread(1, m), q), -4), q)
                total = (sq[m] + q) + (beside + pltpu.roll(up, 1, 0)) + (pltpu.roll(down, 7, 0) + zsum)
                red = total * jnp.float32(SIXTH)
                er[m] = swapped(red, red)

        if not final:
            for sx in range(2):

                @pl.when(has[sx])
                def _():
                    msg_x(sx, t).wait_send()

        with jax.named_scope("P3blk"):
            for m in range(nm):
                v = er[m]
                for sy, g in ((0, 0), (1, ng - 1)):
                    y = tile(1, m, g, edge_at(v, g))
                    put(m, g, y, final)
                    if not final:
                        keep_rows(t + 1, m, g, y, sy)

        if not final:
            send_far(t + 1)
        with jax.named_scope("P4"):
            for m in edge_m:
                black_plane(m, inner, final)
        if not final:
            send_x(t + 1)

        with jax.named_scope("P5"):
            several(1, nm - 1, 3, lambda m: black_plane(m, inner, final))
        if not final:
            with jax.named_scope("pack"):
                pack(t + 1)
            send_z(t + 1)

    for sy in range(2):
        msg_sy(sy).wait_send()
    for zd in range(nz):
        msg_sz(zd).wait_send()
    for t in range(SWEEPS):
        for sy in range(2):
            msg_y(sy, t).wait_send()
            for zd in range(nz):
                msg_yz(sy, zd, t).wait_send()
        for zd in range(nz):
            msg_z(zd, t).wait_send()
    for sx in range(2):

        @pl.when(has[sx])
        def _():
            msg_sx(sx).wait_send()
            msg_x(sx, SWEEPS - 1).wait_send()
            for t in range(SWEEPS):
                for sy in range(2):
                    msg_xy(sx, sy, t).wait_send()
                for zd in range(nz):
                    msg_xz(sx, zd, t).wait_send()


def solution(mesh):
    sizes = tuple(mesh.shape[a] for a in ("gx", "gy", "gz"))

    def on_device(field, source):
        planes, rows, cols = field.shape
        nm, ng, nz = planes // 2, rows // 8, 1 if sizes[2] == 2 else 2
        assert planes % 4 == 0 and nm >= 4 and rows % 8 == 0 and cols == 128 and 4 * ng <= cols
        f32 = jnp.float32
        vm = lambda *shape: pltpu.VMEM(shape, f32)
        return pl.pallas_call(
            functools.partial(kernel, sizes),
            out_shape=jax.ShapeDtypeStruct(field.shape, f32),
            in_specs=[pl.BlockSpec(memory_space=pltpu.HBM)] * 2,
            out_specs=pl.BlockSpec(memory_space=pltpu.VMEM),
            scratch_shapes=[
                vm(*field.shape),
                vm(*field.shape),
                vm(nm + 2, rows + 2 * PAD, cols),
                vm(nm + 2, rows + 2 * PAD, cols),
                vm(nm + 2, rows + 2 * PAD, cols),
                vm(nm, rows + 2 * PAD, cols),
                vm(nm + 2, 8, cols),
                vm(nm, 8, cols),
                vm(nm + 2, 8, cols),
                vm(nm, 8, cols),
                vm(4, nm, cols),
                vm(nm, 8, cols),
                vm(SWEEPS, nm, 8, cols),
                vm(2, SWEEPS, nm, 2, cols),
                vm(2, SWEEPS, nm, cols),
                vm(2, nm, cols),
                vm(2, SWEEPS, rows, cols),
                vm(2, SWEEPS, nm, 2, cols),
                vm(nz, SWEEPS, nm, 8, cols),
                vm(2, 2, SWEEPS, 2, cols),
                vm(2, nz, SWEEPS, nm, cols),
                vm(2, nz, SWEEPS, 8, cols),
                vm(2, nm, cols),
                vm(nz, nm, 8, cols),
                pltpu.SemaphoreType.DMA((24, SWEEPS)),
                pltpu.SemaphoreType.DMA((24, SWEEPS)),
                pltpu.SemaphoreType.DMA((nm + 2,)),
                pltpu.SemaphoreType.DMA((nm,)),
            ],
            compiler_params=pltpu.CompilerParams(
                collective_id=0, has_side_effects=True, vmem_limit_bytes=50 * 1024 * 1024
            ),
        )(field, source)

    spec = P("gx", "gy", "gz")
    return jax.shard_map(on_device, mesh=mesh, in_specs=(spec, spec), out_specs=spec, check_vma=False)
```

```python
import functools

import jax
import jax.numpy as jnp
from jax import lax
from jax.experimental import pallas as pl
from jax.experimental.pallas import tpu as pltpu
from jax.sharding import PartitionSpec as P

SWEEPS = 3
MESH = pl.DeviceIdType.MESH
PAD = 16


def slots(nz):
    sizes = dict(X=4, Y=2, Z=4 * nz, XY=4, YZ=2 * nz, XZ=2 * nz, SX=2, SY=2, SZ=nz)
    first, total = {}, 0
    for name, size in sizes.items():
        if name == "SX":
            rounds = total
        first[name], total = total, total + size
    return first, rounds, total

SIXTH = 1.0 / 6.0


def kernel(
    sizes, f_hbm, s_hbm, ov, fv, sv, x0, x1, s0, s1, eb, er, rq, qb, sq, yzb, sqs,
    pk, jb, yzs, sys_, sxs, sxr, xg, jr, zr, xyr, yzr, xzr, syr, szr, send, recv, fsem, ssem,
):
    ngx, ngy, ngz = sizes
    planes, rows, cols = f_hbm.shape
    nm = planes // 2
    ng = rows // 8
    gx, gy, gz = (lax.axis_index(a) for a in ("gx", "gy", "gz"))
    has = (gx > 0, gx < ngx - 1)
    nz = 1 if ngz == 2 else 2
    y_to = (lax.rem(gy + ngy - 1, ngy), lax.rem(gy + 1, ngy))
    z_to = (lax.rem(gz + 1, ngz), lax.rem(gz + ngz - 1, ngz))[:nz]
    x_to = (gx - 1, gx + 1)
    last = cols - 1
    edge_m = (0, nm - 1)
    mid = nm // 2
    parts = ((0, 1), (nm - 1, nm), (1, mid), (mid, nm - 1))
    middle = parts[2:]

    def load_source(part):
        lo, hi = parts[part]
        at = pl.ds(2 * lo, 2 * (hi - lo))
        return pltpu.make_async_copy(s_hbm.at[at], sv.at[at], ssem.at[part])

    def load_ends(sy):
        rs = pl.ds((0, rows - 8)[sy], 8)
        return pltpu.make_async_copy(f_hbm.at[:, rs], fv.at[:, rs], fsem.at[4 + sy])

    def load_field(part):
        lo, hi = parts[part]
        at = (pl.ds(2 * lo, 2 * (hi - lo)), pl.ds(8, rows - 16))
        return pltpu.make_async_copy(f_hbm.at[at], fv.at[at], fsem.at[part])

    for sy in range(2):
        load_ends(sy).start()
    for part in range(4):
        load_field(part).start()
    for part in range(4):
        load_source(part).start()

    barrier = pltpu.get_barrier_semaphore()

    def greet(device):
        pl.semaphore_signal(barrier, inc=1, device_id=device, device_id_type=MESH)

    for y in y_to:
        greet({"gy": y})
        for z in z_to:
            greet({"gy": y, "gz": z})
    for z in z_to:
        greet({"gz": z})
    for sx in range(2):

        @pl.when(has[sx])
        def _():
            greet({"gx": x_to[sx]})
            for y in y_to:
                greet({"gx": x_to[sx], "gy": y})
            for z in z_to:
                greet({"gx": x_to[sx], "gz": z})

    sub = lax.broadcasted_iota(jnp.int32, (8, cols), 0)
    lane = lax.broadcasted_iota(jnp.int32, (8, cols), 1)
    odd = lax.rem(sub + lane, 2) == 1
    first, final_lane = lane == 0, lane == last
    quad = lax.div(lane, 4)
    pos = lax.rem(lane, 4)
    pos0, pos1, pos3, low_half = pos == 0, pos == 1, pos == 3, pos < 2
    odd_q = lax.rem(sub + jnp.where(pos1, 1, 0), 2) == 1
    top, bottom = sub == 0, sub == 7
    no_up = top & (quad == 0)
    no_down = bottom & (quad == ng - 1)
    ends = first | final_lane
    odd_lane = lax.rem(lax.broadcasted_iota(jnp.int32, (rows // 2, cols), 1), 2) == 1
    zero = jnp.zeros((8, cols), jnp.float32)

    def roll(v, by):
        by = by % cols
        return v if by == 0 else pltpu.roll(v, by, 1)

    for sx in range(2):
        m = (0, nm + 1)[sx]

        @pl.when(jnp.logical_not(has[sx]))
        def _():
            for c in range(2):
                (x0, x1)[c][m] = jnp.zeros((rows + 2 * PAD, cols), jnp.float32)
            eb[m] = zero
            qb[m] = zero

    base, rounds, total_slots = slots(nz)

    def copy(src_ref, dst_ref, device, kind, k, t):
        slot = base[kind] + k
        return pltpu.make_async_remote_copy(
            src_ref=src_ref, dst_ref=dst_ref, send_sem=send.at[slot], recv_sem=recv.at[slot + (t % 2) * total_slots],
            device_id=device, device_id_type=MESH,
        )


    def msg_x(sx, half, t):
        start = half * (rows // 2)
        return copy(
            x1.at[edge_m[sx] + 1, pl.ds(PAD + start, rows // 2)], xg.at[1 - sx, t, pl.ds(start, rows // 2)],
            {"gx": x_to[sx]}, "X", 2 * sx + half, t,
        )

    def msg_y(sy, t):
        return copy(jb.at[sy, t], jr.at[1 - sy, t], {"gy": y_to[sy]}, "Y", sy, t)

    def msg_z(zd, part, t):
        lo, hi = parts[part]
        at = pl.ds(lo, hi - lo)
        return copy(pk.at[t, at], zr.at[zd, t, at], {"gz": z_to[zd]}, "Z", 4 * zd + part, t)

    def msg_xy(sx, sy, t):
        return copy(
            jb.at[sy, t, edge_m[sx]], xyr.at[1 - sx, 1 - sy, t], {"gx": x_to[sx], "gy": y_to[sy]}, "XY", 2 * sx + sy, t
        )

    def msg_yz(sy, zd, t):
        return copy(yzs.at[sy, t], yzr.at[1 - sy, zd, t], {"gy": y_to[sy], "gz": z_to[zd]}, "YZ", nz * sy + zd, t)

    def msg_xz(sx, zd, t):
        return copy(
            pk.at[t, edge_m[sx]], xzr.at[1 - sx, zd, t], {"gx": x_to[sx], "gz": z_to[zd]}, "XZ", nz * sx + zd, t
        )

    def msg_sx(sx):
        return copy(sxs.at[sx], sxr.at[1 - sx], {"gx": x_to[sx]}, "SX", sx, 0)

    def source_face(sx):
        even = s0[edge_m[sx] + 1, pl.ds(PAD, rows // 2, stride=2), :]
        uneven = s0[edge_m[sx] + 1, pl.ds(PAD + 1, rows // 2, stride=2), :]
        sxs[sx] = jnp.where(odd_lane, uneven, even) if sx == 0 else jnp.where(odd_lane, even, uneven)

    def msg_sy(sy):
        return copy(sys_.at[sy], syr.at[1 - sy], {"gy": y_to[sy]}, "SY", sy, 0)

    def msg_sz(zd):
        return copy(sqs, szr.at[zd], {"gz": z_to[zd]}, "SZ", zd, 0)

    def send_far(t):
        for sy in range(2):
            for zd in range(nz):
                msg_yz(sy, zd, t).start()
        for sx in range(2):

            @pl.when(has[sx])
            def _():
                for sy in range(2):
                    msg_xy(sx, sy, t).start()

        for sy in range(2):
            msg_y(sy, t).start()

    def send_x(half, t):
        for sx in range(2):

            @pl.when(has[sx])
            def _():
                msg_x(sx, half, t).start()

    def send_z(part, t):
        for zd in range(nz):
            msg_z(zd, part, t).start()

    def send_edges(t):
        for sx in range(2):

            @pl.when(has[sx])
            def _():
                for zd in range(nz):
                    msg_xz(sx, zd, t).start()

        for part in range(2):
            send_z(part, t)

    def sent(t):
        for sy in range(2):
            msg_y(sy, t).wait_send()
            if t == 0:
                msg_sy(sy).wait_send()
            for zd in range(nz):
                msg_yz(sy, zd, t).wait_send()
        for zd in range(nz):
            if t == 0:
                msg_sz(zd).wait_send()
            for part in range(4):
                msg_z(zd, part, t).wait_send()
        for sx in range(2):

            @pl.when(has[sx])
            def _():
                if t == 0:
                    msg_sx(sx).wait_send()
                for half in range(2):
                    msg_x(sx, half, t).wait_send()
                for sy in range(2):
                    msg_xy(sx, sy, t).wait_send()
                for zd in range(nz):
                    msg_xz(sx, zd, t).wait_send()

    def rows_of(g, shift=0):
        return pl.ds(PAD + 8 * g + shift, 8)

    def keep_rows(t, m, y, sy):
        jb[sy, t, m] = y[0:2] if sy == 0 else y[6:8]
        yzs[sy, t, pl.ds(m, 1), :] = y[0:1] if sy == 0 else y[7:8]

    def packed(acc, g, y):
        return jnp.where(quad == g, roll(y, 4 * g + 2), acc)

    def field_rows(m, groups):
        for g in groups:
            rs = pl.ds(8 * g, 8)
            x1[m + 1, rows_of(g), :] = jnp.where(odd, fv[2 * m, rs, :], fv[2 * m + 1, rs, :])

    def field_plane(m):
        field_rows(m, inner)

    def several(lo, hi, n, body):
        n = max(k for k in range(1, n + 1) if (hi - lo) % k == 0)

        def step(i, carry):
            for k in range(n):
                body(lo + n * i + k)
            return carry

        lax.fori_loop(0, (hi - lo) // n, step, 0)

    def pack_plane(t, m):
        acc = [zero] * 4
        for g in range(ng):
            acc[g % 4] = packed(acc[g % 4], g, x1[m + 1, rows_of(g), :])
        pk[t, m] = (acc[0] + acc[1]) + (acc[2] + acc[3])

    def pack(part, t):
        with jax.named_scope("pack"):
            several(*middle[part], 4, functools.partial(pack_plane, t))
        send_z(2 + part, t)

    def pack_edges(t):
        with jax.named_scope("packe"):
            for m in edge_m:
                pack_plane(t, m)
        send_edges(t)

    inner = range(1, ng - 1)

    def source_plane(m):
        acc = [zero] * 4
        for g in range(ng):
            rs = pl.ds(8 * g, 8)
            low, high = sv[2 * m, rs, :], sv[2 * m + 1, rs, :]
            red = jnp.where(odd, high, low)
            s0[m + 1, rows_of(g), :] = red
            s1[m, rows_of(g), :] = jnp.where(odd, low, high)
            acc[g % 4] = packed(acc[g % 4], g, red)
            if g == 0:
                sys_[0, pl.ds(m, 1), :] = red[0:1]
            if g == ng - 1:
                sys_[1, pl.ds(m, 1), :] = red[7:8]
        sqs[m] = (acc[0] + acc[1]) + (acc[2] + acc[3])

    with jax.named_scope("ends"):
        for sy, g in ((0, 0), (1, ng - 1)):
            load_ends(sy).wait()
            for m in range(nm):
                field_rows(m, (g,))
                keep_rows(0, m, x1[m + 1, rows_of(g), :], sy)
    near = [h.astype(jnp.int32) for h in has]
    with jax.named_scope("barrier"):
        pl.semaphore_wait(barrier, 2 + 3 * nz + (near[0] + near[1]) * (3 + nz))
    send_far(0)
    with jax.named_scope("field"):
        for part in range(2):
            load_field(part).wait()
            field_plane(edge_m[part])
        for half in range(2):
            send_x(half, 0)
    pack_edges(0)
    for part in range(2):
        with jax.named_scope("field"):
            load_field(2 + part).wait()
            several(*middle[part], 3, field_plane)
        pack(part, 0)
    with jax.named_scope("source"):
        for part in range(4):
            load_source(part).wait()
        several(0, nm, 4, source_plane)
    for sx in range(2):

        @pl.when(has[sx])
        def _():
            source_face(sx)
            msg_sx(sx).start()

    for sy in range(2):
        msg_sy(sy).start()
    for zd in range(nz):
        msg_sz(zd).start()

    def tile(c, m, g, edge, side=None, right=None):
        v = (x1, x0)[c]
        rs = rows_of(g)
        here = v[m + 1, rs, :]
        if side is None:
            below, above = v[m, rs, :], v[m + 2, rs, :]
            beside = jnp.where(odd, above, below) if c == 0 else jnp.where(odd, below, above)
        else:
            beside = v[m + 1 + side, rs, :]
        given = s0[m + 1, rs, :] if c == 0 else s1[m, rs, :]
        total = (given + here) + (beside + v[m + 1, rows_of(g, -1), :])
        total = total + v[m + 1, rows_of(g, 1), :]
        total = total + jnp.where(first, edge, roll(here, 1))
        total = total + jnp.where(final_lane, edge if right is None else right, roll(here, -1))
        return total * jnp.float32(SIXTH)

    def edge_at(v, g):
        return roll(v, -(4 * g + 2))

    def red_plane(m, groups, side=None):
        v = eb[m + 1]
        for g in groups:
            x0[m + 1, rows_of(g), :] = tile(0, m, g, edge_at(v, g), side)

    def put(m, g, y, final):
        if final:
            red = x0[m + 1, rows_of(g), :]
            rs = pl.ds(8 * g, 8)
            ov[2 * m, rs, :] = jnp.where(odd, y, red)
            ov[2 * m + 1, rs, :] = jnp.where(odd, red, y)
        else:
            x1[m + 1, rows_of(g), :] = y

    def black_plane(m, groups, final):
        v = er[m]
        for g in groups:
            put(m, g, tile(1, m, g, edge_at(v, g)), final)

    def swapped(lo, hi):
        return jnp.where(pos1, roll(hi, -1), roll(lo, 1))

    lane8 = lax.broadcasted_iota(jnp.int32, (nm, cols), 1)
    hi_z = nz - 1

    def ghost_plane(sx, groups):
        m = (-1, nm)[sx]
        v = eb[m + 1]
        for g in groups:
            y = tile(0, m, g, edge_at(v, g), (1, -1)[sx])
            x0[m + 1, rows_of(g), :] = jnp.where(has[sx], y, 0.0)

    def take_z(part, t):
        with jax.named_scope("waitz"):
            for zd in range(nz):
                msg_z(zd, part, t).wait_recv()
        for m in range(*parts[part]):
            lo, hi = zr[0, t, m], zr[hi_z, t, m]
            qb[m + 1] = jnp.where(low_half, lo, hi)
            eb[m + 1] = swapped(lo, hi)

    z_early = lax.rem(gx, 2) == 1

    def close_inner(t):
        for part in range(2):
            take_z(2 + part, t)
            with jax.named_scope("P1z"):
                several(*middle[part], 3, close_plane)

    def pre_red(t):
        if t == 0:
            for zd in range(nz):
                msg_sz(zd).wait_recv()
            for m in range(nm):
                sq[m] = jnp.where(low_half, szr[0, m], szr[hi_z, m])
        for m in range(nm):
            own, q = pk[t, m], qb[m + 1]
            zsum = roll(jnp.where(pos0, q, own), 1) + roll(jnp.where(pos3, q, own), -1)
            beside = jnp.where(odd_q, qb[m + 2], qb[m])
            up = jnp.where(bottom, roll(q, 4), q)
            up = jnp.where(no_up, 0.0, pltpu.roll(up, 1, 0))
            down = jnp.where(top, roll(q, -4), q)
            down = jnp.where(no_down, 0.0, pltpu.roll(down, 7, 0))
            rq[m] = (sq[m] + q) + (beside + up) + (down + zsum)

    def open_plane(m):
        for g in inner:
            x0[m + 1, rows_of(g), :] = tile(0, m, g, 0.0)

    def close_plane(m):
        v = eb[m + 1] * jnp.float32(SIXTH)
        for g in inner:
            rs = rows_of(g)
            x0[m + 1, rs, :] = x0[m + 1, rs, :] + jnp.where(ends, edge_at(v, g), 0.0)

    for t in range(SWEEPS):
        final = t == SWEEPS - 1
        with jax.named_scope("P1"):
            several(1, nm - 1, 3, open_plane)
        with jax.named_scope("sent"):
            sent(t)
        for part in range(2):
            take_z(part, t)

        @pl.when(z_early)
        def _():
            close_inner(t)

        for half in range(2):
            start = half * (rows // 2)
            groups = (inner[: ng // 2 - 2], inner[ng // 2 - 2 :])[half]
            with jax.named_scope("waitx"):
                for sx in range(2):
                    at = (0, nm + 1)[sx]

                    @pl.when(has[sx])
                    def _():
                        if half == 0:
                            for zd in range(nz):
                                msg_xz(1 - sx, zd, t).wait_recv()
                            lo, hi = xzr[sx, 0, t], xzr[sx, hi_z, t]
                            qb[at] = jnp.where(low_half, lo, hi)
                            eb[at] = swapped(lo, hi)
                            if t == 0:
                                msg_sx(1 - sx).wait_recv()
                                for row in range(2):
                                    s0[at, pl.ds(PAD + row, rows // 2, stride=2), :] = sxr[sx]
                        msg_x(1 - sx, half, t).wait_recv()
                        x1[at, pl.ds(PAD + start, rows // 2), :] = xg[sx, t, pl.ds(start, rows // 2), :]

            with jax.named_scope("P2"):
                for sx in range(2):
                    ghost_plane(sx, groups)
                    red_plane(edge_m[sx], groups)

        @pl.when(jnp.logical_not(z_early))
        def _():
            close_inner(t)

        with jax.named_scope("prered"):
            pre_red(t)

        with jax.named_scope("waity"):
            for sy in range(2):
                if t == 0:
                    msg_sy(sy).wait_recv()
                    for m in range(nm):
                        s0[m + 1, pl.ds((PAD + rows, PAD - 1)[sy], 1), :] = syr[1 - sy, pl.ds(m, 1), :]
                msg_y(sy, t).wait_recv()
                for m in range(nm):
                    x1[m + 1, pl.ds((PAD + rows, PAD - 2)[sy], 2), :] = jr[1 - sy, t, m]
        with jax.named_scope("P3a"):
            for m in range(nm):
                red_plane(m, (0, ng - 1))
        with jax.named_scope("waitfar"):
            for sx in range(2):

                @pl.when(has[sx])
                def _():
                    for sy in range(2):
                        msg_xy(1 - sx, sy, t).wait_recv()
                        x1[(0, nm + 1)[sx], pl.ds((PAD + rows, PAD - 2)[sy], 2), :] = xyr[sx, 1 - sy, t]

            for sy in range(2):
                for zd in range(nz):
                    msg_yz(sy, zd, t).wait_recv()

        with jax.named_scope("P3b"):
            for side in range(2):
                lo, hi = yzr[side, 0, t], yzr[side, hi_z, t]
                yzb[side] = pltpu.roll(jnp.where(lane8 >= cols // 2, lo, hi), (2, (4 * ng - 2) % cols)[side], 1)
                yzb[2 + side] = jnp.where(lane8 == 0, pltpu.roll(lo, 1, 1), pltpu.roll(hi, last, 1))
            for sx in range(2):
                ghost_plane(sx, (0, ng - 1))
            for m in range(nm):
                for g, k in ((-1, 2), (ng, 3)):
                    x0[m + 1, rows_of(g), :] = tile(0, m, g, jnp.broadcast_to(yzb[k, pl.ds(m, 1), :], (8, cols)))
            for m in range(nm):
                total = rq[m] + jnp.where(no_up, jnp.broadcast_to(yzb[0, pl.ds(m, 1), :], (8, cols)), 0.0)
                total = total + jnp.where(no_down, jnp.broadcast_to(yzb[1, pl.ds(m, 1), :], (8, cols)), 0.0)
                rq[m] = total * jnp.float32(SIXTH)
            for m in range(nm):
                red = rq[m]
                for sy, g in ((0, 0), (1, ng - 1)):
                    y = tile(1, m, g, roll(red, -(4 * g + 1)), None, roll(red, -(4 * g + 3)))
                    put(m, g, y, final)
                    if not final:
                        keep_rows(t + 1, m, y, sy)

        if not final:
            send_far(t + 1)
        with jax.named_scope("P4"):
            for m in range(nm):
                er[m] = swapped(rq[m], rq[m])
            for half, groups in enumerate((inner[: ng // 2 - 1], inner[ng // 2 - 1 :])):
                for m in edge_m:
                    black_plane(m, groups, final)
                if not final:
                    send_x(half, t + 1)
        if not final:
            pack_edges(t + 1)
        for part in range(2):
            with jax.named_scope("P5"):
                several(*middle[part], 3, lambda m: black_plane(m, inner, final))
            if not final:
                pack(part, t + 1)


def solution(mesh):
    sizes = tuple(mesh.shape[a] for a in ("gx", "gy", "gz"))

    def on_device(field, source):
        planes, rows, cols = field.shape
        nm, ng, nz = planes // 2, rows // 8, 1 if sizes[2] == 2 else 2
        assert planes % 4 == 0 and nm >= 4 and rows % 8 == 0 and cols == 128 and 4 * ng <= cols
        _, rounds, total_slots = slots(nz)
        f32 = jnp.float32
        vm = lambda *shape: pltpu.VMEM(shape, f32)
        return pl.pallas_call(
            functools.partial(kernel, sizes),
            out_shape=jax.ShapeDtypeStruct(field.shape, f32),
            in_specs=[pl.BlockSpec(memory_space=pltpu.HBM)] * 2,
            out_specs=pl.BlockSpec(memory_space=pltpu.VMEM),
            scratch_shapes=[
                vm(*field.shape),
                vm(*field.shape),
                vm(nm + 2, rows + 2 * PAD, cols),
                vm(nm + 2, rows + 2 * PAD, cols),
                vm(nm + 2, rows + 2 * PAD, cols),
                vm(nm, rows + 2 * PAD, cols),
                vm(nm + 2, 8, cols),
                vm(nm, 8, cols),
                vm(nm, 8, cols),
                vm(nm + 2, 8, cols),
                vm(nm, 8, cols),
                vm(4, nm, cols),
                vm(nm, 8, cols),
                vm(SWEEPS, nm, 8, cols),
                vm(2, SWEEPS, nm, 2, cols),
                vm(2, SWEEPS, nm, cols),
                vm(2, nm, cols),
                vm(2, rows // 2, cols),
                vm(2, rows // 2, cols),
                vm(2, SWEEPS, rows, cols),
                vm(2, SWEEPS, nm, 2, cols),
                vm(nz, SWEEPS, nm, 8, cols),
                vm(2, 2, SWEEPS, 2, cols),
                vm(2, nz, SWEEPS, nm, cols),
                vm(2, nz, SWEEPS, 8, cols),
                vm(2, nm, cols),
                vm(nz, nm, 8, cols),
                pltpu.SemaphoreType.DMA((total_slots,)),
                pltpu.SemaphoreType.DMA((total_slots + rounds,)),
                pltpu.SemaphoreType.DMA((6,)),
                pltpu.SemaphoreType.DMA((4,)),
            ],
            compiler_params=pltpu.CompilerParams(
                collective_id=0, has_side_effects=True, vmem_limit_bytes=50 * 1024 * 1024
            ),
        )(field, source)

    spec = P("gx", "gy", "gz")
    return jax.shard_map(on_device, mesh=mesh, in_specs=(spec, spec), out_specs=spec, check_vma=False)
```

```python
import functools

import jax
import jax.numpy as jnp
from jax import lax
from jax.experimental import pallas as pl
from jax.experimental.pallas import tpu as pltpu
from jax.sharding import PartitionSpec as P

SWEEPS = 3
MESH = pl.DeviceIdType.MESH
PAD = 16


def slots(nz):
    sizes = dict(X=4, Y=2, Z=4 * nz, XY=4, YZ=2 * nz, XZ=2 * nz, SX=2, SY=2, SZ=nz)
    first, total = {}, 0
    for name, size in sizes.items():
        if name == "SX":
            rounds = total
        first[name], total = total, total + size
    return first, rounds, total

SIXTH = 1.0 / 6.0


def kernel(
    sizes, f_hbm, s_hbm, ov, fv, sv, x0, x1, s0, s1, eb, er, rq, qb, sq, yzb, sqs,
    pk, jb, yzs, sys_, sxs, sxr, xg, jr, zr, xyr, yzr, xzr, syr, szr, send, recv, fsem, ssem,
):
    ngx, ngy, ngz = sizes
    planes, rows, cols = f_hbm.shape
    nm = planes // 2
    ng = rows // 8
    gx, gy, gz = (lax.axis_index(a) for a in ("gx", "gy", "gz"))
    has = (gx > 0, gx < ngx - 1)
    nz = 1 if ngz == 2 else 2
    y_to = (lax.rem(gy + ngy - 1, ngy), lax.rem(gy + 1, ngy))
    z_to = (lax.rem(gz + 1, ngz), lax.rem(gz + ngz - 1, ngz))[:nz]
    x_to = (gx - 1, gx + 1)
    last = cols - 1
    edge_m = (0, nm - 1)
    mid = nm // 2
    parts = ((0, 1), (nm - 1, nm), (1, mid), (mid, nm - 1))
    middle = parts[2:]

    def load_source(part):
        lo, hi = parts[part]
        at = pl.ds(2 * lo, 2 * (hi - lo))
        return pltpu.make_async_copy(s_hbm.at[at], sv.at[at], ssem.at[part])

    def load_ends(sy):
        rs = pl.ds((0, rows - 8)[sy], 8)
        return pltpu.make_async_copy(f_hbm.at[:, rs], fv.at[:, rs], fsem.at[4 + sy])

    def load_field(part):
        lo, hi = parts[part]
        at = (pl.ds(2 * lo, 2 * (hi - lo)), pl.ds(8, rows - 16))
        return pltpu.make_async_copy(f_hbm.at[at], fv.at[at], fsem.at[part])

    for sy in range(2):
        load_ends(sy).start()
    for part in range(4):
        load_field(part).start()
    for part in range(4):
        load_source(part).start()

    barrier = pltpu.get_barrier_semaphore()

    def greet(device):
        pl.semaphore_signal(barrier, inc=1, device_id=device, device_id_type=MESH)

    for y in y_to:
        greet({"gy": y})
        for z in z_to:
            greet({"gy": y, "gz": z})
    for z in z_to:
        greet({"gz": z})
    for sx in range(2):

        @pl.when(has[sx])
        def _():
            greet({"gx": x_to[sx]})
            for y in y_to:
                greet({"gx": x_to[sx], "gy": y})
            for z in z_to:
                greet({"gx": x_to[sx], "gz": z})

    sub = lax.broadcasted_iota(jnp.int32, (8, cols), 0)
    lane = lax.broadcasted_iota(jnp.int32, (8, cols), 1)
    odd = lax.rem(sub + lane, 2) == 1
    first, final_lane = lane == 0, lane == last
    quad = lax.div(lane, 4)
    pos = lax.rem(lane, 4)
    pos0, pos1, pos3, low_half = pos == 0, pos == 1, pos == 3, pos < 2
    odd_q = lax.rem(sub + jnp.where(pos1, 1, 0), 2) == 1
    top, bottom = sub == 0, sub == 7
    no_up = top & (quad == 0)
    no_down = bottom & (quad == ng - 1)
    ends = first | final_lane
    odd_lane = lax.rem(lax.broadcasted_iota(jnp.int32, (rows // 2, cols), 1), 2) == 1
    zero = jnp.zeros((8, cols), jnp.float32)

    def roll(v, by):
        by = by % cols
        return v if by == 0 else pltpu.roll(v, by, 1)

    for sx in range(2):
        m = (0, nm + 1)[sx]

        @pl.when(jnp.logical_not(has[sx]))
        def _():
            for c in range(2):
                (x0, x1)[c][m] = jnp.zeros((rows + 2 * PAD, cols), jnp.float32)
            eb[m] = zero
            qb[m] = zero

    base, rounds, total_slots = slots(nz)

    def copy(src_ref, dst_ref, device, kind, k, t):
        slot = base[kind] + k
        return pltpu.make_async_remote_copy(
            src_ref=src_ref, dst_ref=dst_ref, send_sem=send.at[slot], recv_sem=recv.at[slot + (t % 2) * total_slots],
            device_id=device, device_id_type=MESH,
        )


    cross = lax.rem(gx, 2)
    near = 1 - cross
    sides = (near, cross)

    def there(sx):
        return jnp.where(sx == 1, gx < ngx - 1, gx > 0)

    def msg_x(sx, half, t):
        start = half * (rows // 2)
        return copy(
            x1.at[sx * (nm - 1) + 1, pl.ds(PAD + start, rows // 2)], xg.at[1 - sx, t, pl.ds(start, rows // 2)],
            {"gx": gx + 2 * sx - 1}, "X", 2 * sx + half, t,
        )

    def msg_y(sy, t):
        return copy(jb.at[sy, t], jr.at[1 - sy, t], {"gy": y_to[sy]}, "Y", sy, t)

    def msg_z(zd, part, t):
        lo, hi = parts[part]
        at = pl.ds(lo, hi - lo)
        return copy(pk.at[t, at], zr.at[zd, t, at], {"gz": z_to[zd]}, "Z", 4 * zd + part, t)

    def msg_xy(sx, sy, t):
        return copy(
            jb.at[sy, t, edge_m[sx]], xyr.at[1 - sx, 1 - sy, t], {"gx": x_to[sx], "gy": y_to[sy]}, "XY", 2 * sx + sy, t
        )

    def msg_yz(sy, zd, t):
        return copy(yzs.at[sy, t], yzr.at[1 - sy, zd, t], {"gy": y_to[sy], "gz": z_to[zd]}, "YZ", nz * sy + zd, t)

    def msg_xz(sx, zd, t):
        return copy(
            pk.at[t, sx * (nm - 1)], xzr.at[1 - sx, zd, t], {"gx": gx + 2 * sx - 1, "gz": z_to[zd]}, "XZ", nz * sx + zd, t
        )

    def msg_sx(sx):
        return copy(sxs.at[sx], sxr.at[1 - sx], {"gx": gx + 2 * sx - 1}, "SX", sx, 0)

    def source_face(sx):
        even = s0[edge_m[sx] + 1, pl.ds(PAD, rows // 2, stride=2), :]
        uneven = s0[edge_m[sx] + 1, pl.ds(PAD + 1, rows // 2, stride=2), :]
        sxs[sx] = jnp.where(odd_lane, uneven, even) if sx == 0 else jnp.where(odd_lane, even, uneven)

    def msg_sy(sy):
        return copy(sys_.at[sy], syr.at[1 - sy], {"gy": y_to[sy]}, "SY", sy, 0)

    def msg_sz(zd):
        return copy(sqs, szr.at[zd], {"gz": z_to[zd]}, "SZ", zd, 0)

    def send_far(t):
        for sy in range(2):
            for zd in range(nz):
                msg_yz(sy, zd, t).start()
        for sx in range(2):

            @pl.when(has[sx])
            def _():
                for sy in range(2):
                    msg_xy(sx, sy, t).start()

        for sy in range(2):
            msg_y(sy, t).start()

    def send_x(sx, half, t):
        @pl.when(there(sx))
        def _():
            msg_x(sx, half, t).start()

    def send_z(part, t):
        for zd in range(nz):
            msg_z(zd, part, t).start()

    def send_edges(t):
        for sx in range(2):

            @pl.when(has[sx])
            def _():
                for zd in range(nz):
                    msg_xz(sx, zd, t).start()

        for part in range(2):
            send_z(part, t)

    def sent(t):
        for sy in range(2):
            msg_y(sy, t).wait_send()
            if t == 0:
                msg_sy(sy).wait_send()
            for zd in range(nz):
                msg_yz(sy, zd, t).wait_send()
        for zd in range(nz):
            if t == 0:
                msg_sz(zd).wait_send()
            for part in range(4):
                msg_z(zd, part, t).wait_send()
        for sx in range(2):

            @pl.when(has[sx])
            def _():
                if t == 0:
                    msg_sx(sx).wait_send()
                for half in range(2):
                    msg_x(sx, half, t).wait_send()
                for sy in range(2):
                    msg_xy(sx, sy, t).wait_send()
                for zd in range(nz):
                    msg_xz(sx, zd, t).wait_send()

    def rows_of(g, shift=0):
        return pl.ds(PAD + 8 * g + shift, 8)

    def keep_rows(t, m, y, sy):
        jb[sy, t, m] = y[0:2] if sy == 0 else y[6:8]
        yzs[sy, t, pl.ds(m, 1), :] = y[0:1] if sy == 0 else y[7:8]

    def packed(acc, g, y):
        return jnp.where(quad == g, roll(y, 4 * g + 2), acc)

    def field_rows(m, groups):
        for g in groups:
            rs = pl.ds(8 * g, 8)
            x1[m + 1, rows_of(g), :] = jnp.where(odd, fv[2 * m, rs, :], fv[2 * m + 1, rs, :])

    def field_plane(m):
        field_rows(m, inner)

    def several(lo, hi, n, body):
        n = max(k for k in range(1, n + 1) if (hi - lo) % k == 0)

        def step(i, carry):
            for k in range(n):
                body(lo + n * i + k)
            return carry

        lax.fori_loop(0, (hi - lo) // n, step, 0)

    def pack_plane(t, m):
        acc = [zero] * 4
        for g in range(ng):
            acc[g % 4] = packed(acc[g % 4], g, x1[m + 1, rows_of(g), :])
        pk[t, m] = (acc[0] + acc[1]) + (acc[2] + acc[3])

    def pack(part, t):
        with jax.named_scope("pack"):
            several(*middle[part], 4, functools.partial(pack_plane, t))
        send_z(2 + part, t)

    def pack_edges(t):
        with jax.named_scope("packe"):
            for m in edge_m:
                pack_plane(t, m)
        send_edges(t)

    inner = range(1, ng - 1)

    def source_plane(m):
        acc = [zero] * 4
        for g in range(ng):
            rs = pl.ds(8 * g, 8)
            low, high = sv[2 * m, rs, :], sv[2 * m + 1, rs, :]
            red = jnp.where(odd, high, low)
            s0[m + 1, rows_of(g), :] = red
            s1[m, rows_of(g), :] = jnp.where(odd, low, high)
            acc[g % 4] = packed(acc[g % 4], g, red)
            if g == 0:
                sys_[0, pl.ds(m, 1), :] = red[0:1]
            if g == ng - 1:
                sys_[1, pl.ds(m, 1), :] = red[7:8]
        sqs[m] = (acc[0] + acc[1]) + (acc[2] + acc[3])

    with jax.named_scope("ends"):
        for sy, g in ((0, 0), (1, ng - 1)):
            load_ends(sy).wait()
            for m in range(nm):
                field_rows(m, (g,))
                keep_rows(0, m, x1[m + 1, rows_of(g), :], sy)
    links = [h.astype(jnp.int32) for h in has]
    with jax.named_scope("barrier"):
        pl.semaphore_wait(barrier, 2 + 3 * nz + (links[0] + links[1]) * (3 + nz))
    send_far(0)
    with jax.named_scope("field"):
        for part in range(2):
            load_field(part).wait()
            field_plane(edge_m[part])
        for sx in (cross, near):
            for half in range(2):
                send_x(sx, half, 0)
    pack_edges(0)
    for part in range(2):
        with jax.named_scope("field"):
            load_field(2 + part).wait()
            several(*middle[part], 3, field_plane)
        pack(part, 0)
    with jax.named_scope("source"):
        for part in range(4):
            load_source(part).wait()
        several(0, nm, 4, source_plane)
    for sx in range(2):

        @pl.when(has[sx])
        def _():
            source_face(sx)
            msg_sx(sx).start()

    for sy in range(2):
        msg_sy(sy).start()
    for zd in range(nz):
        msg_sz(zd).start()

    def tile(c, m, g, edge, side=None, right=None):
        v = (x1, x0)[c]
        rs = rows_of(g)
        here = v[m + 1, rs, :]
        if side is None:
            below, above = v[m, rs, :], v[m + 2, rs, :]
            beside = jnp.where(odd, above, below) if c == 0 else jnp.where(odd, below, above)
        else:
            beside = v[m + 1 + side, rs, :]
        given = s0[m + 1, rs, :] if c == 0 else s1[m, rs, :]
        total = (given + here) + (beside + v[m + 1, rows_of(g, -1), :])
        total = total + v[m + 1, rows_of(g, 1), :]
        total = total + jnp.where(first, edge, roll(here, 1))
        total = total + jnp.where(final_lane, edge if right is None else right, roll(here, -1))
        return total * jnp.float32(SIXTH)

    def edge_at(v, g):
        return roll(v, -(4 * g + 2))

    def red_plane(m, groups, side=None):
        v = eb[m + 1]
        for g in groups:
            x0[m + 1, rows_of(g), :] = tile(0, m, g, edge_at(v, g), side)

    def put(m, g, y, final):
        if final:
            red = x0[m + 1, rows_of(g), :]
            rs = pl.ds(8 * g, 8)
            ov[2 * m, rs, :] = jnp.where(odd, y, red)
            ov[2 * m + 1, rs, :] = jnp.where(odd, red, y)
        else:
            x1[m + 1, rows_of(g), :] = y

    def black_plane(m, groups, final):
        v = er[m]
        for g in groups:
            put(m, g, tile(1, m, g, edge_at(v, g)), final)

    def swapped(lo, hi):
        return jnp.where(pos1, roll(hi, -1), roll(lo, 1))

    lane8 = lax.broadcasted_iota(jnp.int32, (nm, cols), 1)
    hi_z = nz - 1

    def ghost_plane(sx, groups):
        m = sx * (nm + 1) - 1
        v = eb[m + 1]
        on = there(sx)
        for g in groups:
            y = tile(0, m, g, edge_at(v, g), 1 - 2 * sx)
            x0[m + 1, rows_of(g), :] = jnp.where(on, y, 0.0)

    def take_z(part, t):
        with jax.named_scope("waitz"):
            for zd in range(nz):
                msg_z(zd, part, t).wait_recv()
        for m in range(*parts[part]):
            lo, hi = zr[0, t, m], zr[hi_z, t, m]
            qb[m + 1] = jnp.where(low_half, lo, hi)
            eb[m + 1] = swapped(lo, hi)

    def take_x(sx, half, t):
        at = sx * (nm + 1)
        rs = pl.ds(half * (rows // 2), rows // 2)

        @pl.when(there(sx))
        def _():
            if half == 0:
                for zd in range(nz):
                    msg_xz(1 - sx, zd, t).wait_recv()
                lo, hi = xzr[sx, 0, t], xzr[sx, hi_z, t]
                qb[at] = jnp.where(low_half, lo, hi)
                eb[at] = swapped(lo, hi)
                if t == 0:
                    msg_sx(1 - sx).wait_recv()
                    for row in range(2):
                        s0[at, pl.ds(PAD + row, rows // 2, stride=2), :] = sxr[sx]
            msg_x(1 - sx, half, t).wait_recv()
            x1[at, pl.ds(PAD + half * (rows // 2), rows // 2), :] = xg[sx, t, rs, :]

    z_early = lax.rem(gx, 2) == 1

    def close_inner(t):
        for part in range(2):
            take_z(2 + part, t)
            with jax.named_scope("P1z"):
                several(*middle[part], 3, close_plane)

    def pre_red(t):
        if t == 0:
            for zd in range(nz):
                msg_sz(zd).wait_recv()
            for m in range(nm):
                sq[m] = jnp.where(low_half, szr[0, m], szr[hi_z, m])
        for m in range(nm):
            own, q = pk[t, m], qb[m + 1]
            zsum = roll(jnp.where(pos0, q, own), 1) + roll(jnp.where(pos3, q, own), -1)
            beside = jnp.where(odd_q, qb[m + 2], qb[m])
            up = jnp.where(bottom, roll(q, 4), q)
            up = jnp.where(no_up, 0.0, pltpu.roll(up, 1, 0))
            down = jnp.where(top, roll(q, -4), q)
            down = jnp.where(no_down, 0.0, pltpu.roll(down, 7, 0))
            rq[m] = (sq[m] + q) + (beside + up) + (down + zsum)

    def open_plane(m):
        for g in inner:
            x0[m + 1, rows_of(g), :] = tile(0, m, g, 0.0)

    def close_plane(m):
        v = eb[m + 1] * jnp.float32(SIXTH)
        for g in inner:
            rs = rows_of(g)
            x0[m + 1, rs, :] = x0[m + 1, rs, :] + jnp.where(ends, edge_at(v, g), 0.0)

    for t in range(SWEEPS):
        final = t == SWEEPS - 1
        with jax.named_scope("P1"):
            several(1, nm - 1, 3, open_plane)
        with jax.named_scope("sent"):
            sent(t)
        for part in range(2):
            take_z(part, t)

        with jax.named_scope("waitxn"):
            for half in range(2):
                take_x(near, half, t)
        with jax.named_scope("P2n"):
            ghost_plane(near, inner)
            red_plane(near * (nm - 1), inner)

        @pl.when(z_early)
        def _():
            close_inner(t)

        for half in range(2):
            groups = (inner[: ng // 2 - 2], inner[ng // 2 - 2 :])[half]
            with jax.named_scope("waitx"):
                take_x(cross, half, t)
            with jax.named_scope("P2"):
                ghost_plane(cross, groups)
                red_plane(cross * (nm - 1), groups)

        @pl.when(jnp.logical_not(z_early))
        def _():
            close_inner(t)

        with jax.named_scope("prered"):
            pre_red(t)

        with jax.named_scope("waity"):
            for sy in range(2):
                if t == 0:
                    msg_sy(sy).wait_recv()
                    for m in range(nm):
                        s0[m + 1, pl.ds((PAD + rows, PAD - 1)[sy], 1), :] = syr[1 - sy, pl.ds(m, 1), :]
                msg_y(sy, t).wait_recv()
                for m in range(nm):
                    x1[m + 1, pl.ds((PAD + rows, PAD - 2)[sy], 2), :] = jr[1 - sy, t, m]
        with jax.named_scope("P3a"):
            for m in range(nm):
                red_plane(m, (0, ng - 1))
        with jax.named_scope("waitfar"):
            for sx in range(2):

                @pl.when(has[sx])
                def _():
                    for sy in range(2):
                        msg_xy(1 - sx, sy, t).wait_recv()
                        x1[(0, nm + 1)[sx], pl.ds((PAD + rows, PAD - 2)[sy], 2), :] = xyr[sx, 1 - sy, t]

            for sy in range(2):
                for zd in range(nz):
                    msg_yz(sy, zd, t).wait_recv()

        with jax.named_scope("P3b"):
            for side in range(2):
                lo, hi = yzr[side, 0, t], yzr[side, hi_z, t]
                yzb[side] = pltpu.roll(jnp.where(lane8 >= cols // 2, lo, hi), (2, (4 * ng - 2) % cols)[side], 1)
                yzb[2 + side] = jnp.where(lane8 == 0, pltpu.roll(lo, 1, 1), pltpu.roll(hi, last, 1))
            for sx in range(2):
                ghost_plane(sx, (0, ng - 1))
            for m in range(nm):
                for g, k in ((-1, 2), (ng, 3)):
                    x0[m + 1, rows_of(g), :] = tile(0, m, g, jnp.broadcast_to(yzb[k, pl.ds(m, 1), :], (8, cols)))
            for m in range(nm):
                total = rq[m] + jnp.where(no_up, jnp.broadcast_to(yzb[0, pl.ds(m, 1), :], (8, cols)), 0.0)
                total = total + jnp.where(no_down, jnp.broadcast_to(yzb[1, pl.ds(m, 1), :], (8, cols)), 0.0)
                rq[m] = total * jnp.float32(SIXTH)
            for m in range(nm):
                red = rq[m]
                for sy, g in ((0, 0), (1, ng - 1)):
                    y = tile(1, m, g, roll(red, -(4 * g + 1)), None, roll(red, -(4 * g + 3)))
                    put(m, g, y, final)
                    if not final:
                        keep_rows(t + 1, m, y, sy)

        if not final:
            send_far(t + 1)
        with jax.named_scope("P4"):
            for m in range(nm):
                er[m] = swapped(rq[m], rq[m])
            for half, groups in enumerate((inner[: ng // 2 - 1], inner[ng // 2 - 1 :])):
                black_plane(cross * (nm - 1), groups, final)
                if not final:
                    send_x(cross, half, t + 1)
            black_plane(near * (nm - 1), inner, final)
            if not final:
                for half in range(2):
                    send_x(near, half, t + 1)
        if not final:
            pack_edges(t + 1)
        for part in range(2):
            with jax.named_scope("P5"):
                several(*middle[part], 3, lambda m: black_plane(m, inner, final))
            if not final:
                pack(part, t + 1)


def solution(mesh):
    sizes = tuple(mesh.shape[a] for a in ("gx", "gy", "gz"))

    def on_device(field, source):
        planes, rows, cols = field.shape
        nm, ng, nz = planes // 2, rows // 8, 1 if sizes[2] == 2 else 2
        assert planes % 4 == 0 and nm >= 4 and rows % 8 == 0 and cols == 128 and 4 * ng <= cols
        _, rounds, total_slots = slots(nz)
        f32 = jnp.float32
        vm = lambda *shape: pltpu.VMEM(shape, f32)
        return pl.pallas_call(
            functools.partial(kernel, sizes),
            out_shape=jax.ShapeDtypeStruct(field.shape, f32),
            in_specs=[pl.BlockSpec(memory_space=pltpu.HBM)] * 2,
            out_specs=pl.BlockSpec(memory_space=pltpu.VMEM),
            scratch_shapes=[
                vm(*field.shape),
                vm(*field.shape),
                vm(nm + 2, rows + 2 * PAD, cols),
                vm(nm + 2, rows + 2 * PAD, cols),
                vm(nm + 2, rows + 2 * PAD, cols),
                vm(nm, rows + 2 * PAD, cols),
                vm(nm + 2, 8, cols),
                vm(nm, 8, cols),
                vm(nm, 8, cols),
                vm(nm + 2, 8, cols),
                vm(nm, 8, cols),
                vm(4, nm, cols),
                vm(nm, 8, cols),
                vm(SWEEPS, nm, 8, cols),
                vm(2, SWEEPS, nm, 2, cols),
                vm(2, SWEEPS, nm, cols),
                vm(2, nm, cols),
                vm(2, rows // 2, cols),
                vm(2, rows // 2, cols),
                vm(2, SWEEPS, rows, cols),
                vm(2, SWEEPS, nm, 2, cols),
                vm(nz, SWEEPS, nm, 8, cols),
                vm(2, 2, SWEEPS, 2, cols),
                vm(2, nz, SWEEPS, nm, cols),
                vm(2, nz, SWEEPS, 8, cols),
                vm(2, nm, cols),
                vm(nz, nm, 8, cols),
                pltpu.SemaphoreType.DMA((total_slots,)),
                pltpu.SemaphoreType.DMA((total_slots + rounds,)),
                pltpu.SemaphoreType.DMA((6,)),
                pltpu.SemaphoreType.DMA((4,)),
            ],
            compiler_params=pltpu.CompilerParams(
                collective_id=0, has_side_effects=True, vmem_limit_bytes=50 * 1024 * 1024
            ),
        )(field, source)

    spec = P("gx", "gy", "gz")
    return jax.shard_map(on_device, mesh=mesh, in_specs=(spec, spec), out_specs=spec, check_vma=False)
```

```python
import functools

import jax
import jax.numpy as jnp
from jax import lax
from jax.experimental import pallas as pl
from jax.experimental.pallas import tpu as pltpu
from jax.sharding import PartitionSpec as P

SWEEPS = 3
MESH = pl.DeviceIdType.MESH
PAD = 16


def slots(nz):
    sizes = dict(X=4, Y=2, Z=4 * nz, XY=4, YZ=2 * nz, XZ=2 * nz, SX=2, SY=2, SZ=nz)
    first, total = {}, 0
    for name, size in sizes.items():
        if name == "SX":
            rounds = total
        first[name], total = total, total + size
    return first, rounds, total

SIXTH = 1.0 / 6.0


def kernel(
    sizes, f_hbm, s_hbm, x0, s1, er, fv, sv, x1, s0, eb, rq, qb, sq, yzb, sqs,
    pk, jb, yzs, sys_, sxs, sxr, xg, jr, zr, xyr, yzr, xzr, syr, szr, send, recv, fsem, ssem,
):
    ngx, ngy, ngz = sizes
    planes, rows, cols = f_hbm.shape
    nm = planes // 2
    ng = rows // 8
    gx, gy, gz = (lax.axis_index(a) for a in ("gx", "gy", "gz"))
    has = (gx > 0, gx < ngx - 1)
    nz = 1 if ngz == 2 else 2
    y_to = (lax.rem(gy + ngy - 1, ngy), lax.rem(gy + 1, ngy))
    z_to = (lax.rem(gz + 1, ngz), lax.rem(gz + ngz - 1, ngz))[:nz]
    x_to = (gx - 1, gx + 1)
    last = cols - 1
    edge_m = (0, nm - 1)
    mid = nm // 2
    parts = ((0, 1), (nm - 1, nm), (1, mid), (mid, nm - 1))
    middle = parts[2:]

    def load_source(part):
        lo, hi = parts[part]
        at = pl.ds(2 * lo, 2 * (hi - lo))
        return pltpu.make_async_copy(s_hbm.at[at], sv.at[at], ssem.at[part])

    def load_ends(sy):
        rs = pl.ds((0, rows - 8)[sy], 8)
        return pltpu.make_async_copy(f_hbm.at[:, rs], fv.at[:, rs], fsem.at[4 + sy])

    def load_field(part):
        lo, hi = parts[part]
        at = (pl.ds(2 * lo, 2 * (hi - lo)), pl.ds(8, rows - 16))
        return pltpu.make_async_copy(f_hbm.at[at], fv.at[at], fsem.at[part])

    for sy in range(2):
        load_ends(sy).start()
    for part in range(4):
        load_field(part).start()
    for part in range(4):
        load_source(part).start()

    barrier = pltpu.get_barrier_semaphore()

    def greet(device):
        pl.semaphore_signal(barrier, inc=1, device_id=device, device_id_type=MESH)

    for y in y_to:
        greet({"gy": y})
        for z in z_to:
            greet({"gy": y, "gz": z})
    for z in z_to:
        greet({"gz": z})
    for sx in range(2):

        @pl.when(has[sx])
        def _():
            greet({"gx": x_to[sx]})
            for y in y_to:
                greet({"gx": x_to[sx], "gy": y})
            for z in z_to:
                greet({"gx": x_to[sx], "gz": z})

    sub = lax.broadcasted_iota(jnp.int32, (8, cols), 0)
    lane = lax.broadcasted_iota(jnp.int32, (8, cols), 1)
    odd = lax.rem(sub + lane, 2) == 1
    first, final_lane = lane == 0, lane == last
    quad = lax.div(lane, 4)
    pos = lax.rem(lane, 4)
    pos0, pos1, pos3, low_half = pos == 0, pos == 1, pos == 3, pos < 2
    odd_q = lax.rem(sub + jnp.where(pos1, 1, 0), 2) == 1
    top, bottom = sub == 0, sub == 7
    no_up = top & (quad == 0)
    no_down = bottom & (quad == ng - 1)
    ends = first | final_lane
    odd_lane = lax.rem(lax.broadcasted_iota(jnp.int32, (rows // 2, cols), 1), 2) == 1
    zero = jnp.zeros((8, cols), jnp.float32)

    def roll(v, by):
        by = by % cols
        return v if by == 0 else pltpu.roll(v, by, 1)

    for sx in range(2):
        m = (0, nm + 1)[sx]

        @pl.when(jnp.logical_not(has[sx]))
        def _():
            for c in range(2):
                (x0, x1)[c][m] = jnp.zeros((rows + 2 * PAD, cols), jnp.float32)
            eb[m] = zero
            qb[m] = zero

    base, rounds, total_slots = slots(nz)

    def copy(src_ref, dst_ref, device, kind, k, t):
        slot = base[kind] + k
        return pltpu.make_async_remote_copy(
            src_ref=src_ref, dst_ref=dst_ref, send_sem=send.at[slot], recv_sem=recv.at[slot + (t % 2) * total_slots],
            device_id=device, device_id_type=MESH,
        )


    cross = lax.rem(gx, 2)
    near = 1 - cross
    sides = (near, cross)

    def there(sx):
        return jnp.where(sx == 1, gx < ngx - 1, gx > 0)

    def msg_x(sx, half, t):
        start = half * (rows // 2)
        return copy(
            x1.at[sx * (nm - 1) + 1, pl.ds(PAD + start, rows // 2)], xg.at[1 - sx, t, pl.ds(start, rows // 2)],
            {"gx": gx + 2 * sx - 1}, "X", 2 * sx + half, t,
        )

    def msg_y(sy, t):
        return copy(jb.at[sy, t], jr.at[1 - sy, t], {"gy": y_to[sy]}, "Y", sy, t)

    def msg_z(zd, part, t):
        lo, hi = parts[part]
        at = pl.ds(lo, hi - lo)
        return copy(pk.at[t, at], zr.at[zd, t, at], {"gz": z_to[zd]}, "Z", 4 * zd + part, t)

    def msg_xy(sx, sy, t):
        return copy(
            jb.at[sy, t, edge_m[sx]], xyr.at[1 - sx, 1 - sy, t], {"gx": x_to[sx], "gy": y_to[sy]}, "XY", 2 * sx + sy, t
        )

    def msg_yz(sy, zd, t):
        return copy(yzs.at[sy, t], yzr.at[1 - sy, zd, t], {"gy": y_to[sy], "gz": z_to[zd]}, "YZ", nz * sy + zd, t)

    def msg_xz(sx, zd, t):
        return copy(
            pk.at[t, sx * (nm - 1)], xzr.at[1 - sx, zd, t], {"gx": gx + 2 * sx - 1, "gz": z_to[zd]}, "XZ", nz * sx + zd, t
        )

    def msg_sx(sx):
        return copy(sxs.at[sx], sxr.at[1 - sx], {"gx": gx + 2 * sx - 1}, "SX", sx, 0)

    def source_face(sx):
        even = s0[edge_m[sx] + 1, pl.ds(PAD, rows // 2, stride=2), :]
        uneven = s0[edge_m[sx] + 1, pl.ds(PAD + 1, rows // 2, stride=2), :]
        sxs[sx] = jnp.where(odd_lane, uneven, even) if sx == 0 else jnp.where(odd_lane, even, uneven)

    def msg_sy(sy):
        return copy(sys_.at[sy], syr.at[1 - sy], {"gy": y_to[sy]}, "SY", sy, 0)

    def msg_sz(zd):
        return copy(sqs, szr.at[zd], {"gz": z_to[zd]}, "SZ", zd, 0)

    def send_far(t):
        for sy in range(2):
            for zd in range(nz):
                msg_yz(sy, zd, t).start()
        for sx in range(2):

            @pl.when(has[sx])
            def _():
                for sy in range(2):
                    msg_xy(sx, sy, t).start()

        for sy in range(2):
            msg_y(sy, t).start()

    def send_x(sx, half, t):
        @pl.when(there(sx))
        def _():
            msg_x(sx, half, t).start()

    def send_z(part, t):
        for zd in range(nz):
            msg_z(zd, part, t).start()

    def send_edges(t):
        for sx in range(2):

            @pl.when(has[sx])
            def _():
                for zd in range(nz):
                    msg_xz(sx, zd, t).start()

        for part in range(2):
            send_z(part, t)

    def sent(t):
        for sy in range(2):
            msg_y(sy, t).wait_send()
            if t == 0:
                msg_sy(sy).wait_send()
            for zd in range(nz):
                msg_yz(sy, zd, t).wait_send()
        for zd in range(nz):
            if t == 0:
                msg_sz(zd).wait_send()
            for part in range(4):
                msg_z(zd, part, t).wait_send()
        for sx in range(2):

            @pl.when(has[sx])
            def _():
                if t == 0:
                    msg_sx(sx).wait_send()
                for half in range(2):
                    msg_x(sx, half, t).wait_send()
                for sy in range(2):
                    msg_xy(sx, sy, t).wait_send()
                for zd in range(nz):
                    msg_xz(sx, zd, t).wait_send()

    def rows_of(g, shift=0):
        return pl.ds(PAD + 8 * g + shift, 8)

    def keep_rows(t, m, y, sy):
        jb[sy, t, m] = y[0:2] if sy == 0 else y[6:8]
        yzs[sy, t, pl.ds(m, 1), :] = y[0:1] if sy == 0 else y[7:8]

    def packed(acc, g, y):
        return jnp.where(quad == g, roll(y, 4 * g + 2), acc)

    def field_rows(m, groups):
        for g in groups:
            rs = pl.ds(8 * g, 8)
            x1[m + 1, rows_of(g), :] = jnp.where(odd, fv[2 * m, rs, :], fv[2 * m + 1, rs, :])

    def field_plane(m):
        field_rows(m, inner)

    def several(lo, hi, n, body):
        n = max(k for k in range(1, n + 1) if (hi - lo) % k == 0)

        def step(i, carry):
            for k in range(n):
                body(lo + n * i + k)
            return carry

        lax.fori_loop(0, (hi - lo) // n, step, 0)

    def pack_plane(t, m):
        acc = [zero] * 4
        for g in range(ng):
            acc[g % 4] = packed(acc[g % 4], g, x1[m + 1, rows_of(g), :])
        pk[t, m] = (acc[0] + acc[1]) + (acc[2] + acc[3])

    def pack(part, t):
        with jax.named_scope("pack"):
            several(*middle[part], 4, functools.partial(pack_plane, t))
        send_z(2 + part, t)

    def pack_edges(t):
        with jax.named_scope("packe"):
            for m in edge_m:
                pack_plane(t, m)
        send_edges(t)

    inner = range(1, ng - 1)

    def source_plane(m):
        acc = [zero] * 4
        for g in range(ng):
            rs = pl.ds(8 * g, 8)
            low, high = sv[2 * m, rs, :], sv[2 * m + 1, rs, :]
            red = jnp.where(odd, high, low)
            s0[m + 1, rows_of(g), :] = red
            s1[m, rows_of(g), :] = jnp.where(odd, low, high)
            acc[g % 4] = packed(acc[g % 4], g, red)
            if g == 0:
                sys_[0, pl.ds(m, 1), :] = red[0:1]
            if g == ng - 1:
                sys_[1, pl.ds(m, 1), :] = red[7:8]
        sqs[m] = (acc[0] + acc[1]) + (acc[2] + acc[3])

    with jax.named_scope("ends"):
        for sy, g in ((0, 0), (1, ng - 1)):
            load_ends(sy).wait()
            for m in range(nm):
                field_rows(m, (g,))
                keep_rows(0, m, x1[m + 1, rows_of(g), :], sy)
    links = [h.astype(jnp.int32) for h in has]
    with jax.named_scope("barrier"):
        pl.semaphore_wait(barrier, 2 + 3 * nz + (links[0] + links[1]) * (3 + nz))
    send_far(0)
    with jax.named_scope("field"):
        for part in range(2):
            load_field(part).wait()
            field_plane(edge_m[part])
        for sx in (cross, near):
            for half in range(2):
                send_x(sx, half, 0)
    pack_edges(0)
    for part in range(2):
        with jax.named_scope("field"):
            load_field(2 + part).wait()
            several(*middle[part], 3, field_plane)
        pack(part, 0)
    with jax.named_scope("source"):
        for part in range(4):
            load_source(part).wait()
        several(0, nm, 4, source_plane)
    for sx in range(2):

        @pl.when(has[sx])
        def _():
            source_face(sx)
            msg_sx(sx).start()

    for sy in range(2):
        msg_sy(sy).start()
    for zd in range(nz):
        msg_sz(zd).start()

    def tile(c, m, g, edge, side=None, right=None):
        v = (x1, x0)[c]
        rs = rows_of(g)
        here = v[m + 1, rs, :]
        if side is None:
            below, above = v[m, rs, :], v[m + 2, rs, :]
            beside = jnp.where(odd, above, below) if c == 0 else jnp.where(odd, below, above)
        else:
            beside = v[m + 1 + side, rs, :]
        given = s0[m + 1, rs, :] if c == 0 else s1[m, rs, :]
        total = (given + here) + (beside + v[m + 1, rows_of(g, -1), :])
        total = total + v[m + 1, rows_of(g, 1), :]
        total = total + jnp.where(first, edge, roll(here, 1))
        total = total + jnp.where(final_lane, edge if right is None else right, roll(here, -1))
        return total * jnp.float32(SIXTH)

    def edge_at(v, g):
        return roll(v, -(4 * g + 2))

    def red_plane(m, groups, side=None):
        v = eb[m + 1]
        for g in groups:
            x0[m + 1, rows_of(g), :] = tile(0, m, g, edge_at(v, g), side)

    def put(m, g, y):
        x1[m + 1, rows_of(g), :] = y

    def black_plane(m, groups):
        v = er[m]
        for g in groups:
            put(m, g, tile(1, m, g, edge_at(v, g)))

    def swapped(lo, hi):
        return jnp.where(pos1, roll(hi, -1), roll(lo, 1))

    lane8 = lax.broadcasted_iota(jnp.int32, (nm, cols), 1)
    hi_z = nz - 1

    def ghost_plane(sx, groups):
        m = sx * (nm + 1) - 1
        v = eb[m + 1]
        on = there(sx)
        for g in groups:
            y = tile(0, m, g, edge_at(v, g), 1 - 2 * sx)
            x0[m + 1, rows_of(g), :] = jnp.where(on, y, 0.0)

    def take_z(part, t):
        with jax.named_scope("waitz"):
            for zd in range(nz):
                msg_z(zd, part, t).wait_recv()
        for m in range(*parts[part]):
            lo, hi = zr[0, t, m], zr[hi_z, t, m]
            qb[m + 1] = jnp.where(low_half, lo, hi)
            eb[m + 1] = swapped(lo, hi)

    def take_x(sx, half, t):
        at = sx * (nm + 1)
        rs = pl.ds(half * (rows // 2), rows // 2)

        @pl.when(there(sx))
        def _():
            if half == 0:
                for zd in range(nz):
                    msg_xz(1 - sx, zd, t).wait_recv()
                lo, hi = xzr[sx, 0, t], xzr[sx, hi_z, t]
                qb[at] = jnp.where(low_half, lo, hi)
                eb[at] = swapped(lo, hi)
                if t == 0:
                    msg_sx(1 - sx).wait_recv()
                    for row in range(2):
                        s0[at, pl.ds(PAD + row, rows // 2, stride=2), :] = sxr[sx]
            msg_x(1 - sx, half, t).wait_recv()
            x1[at, pl.ds(PAD + half * (rows // 2), rows // 2), :] = xg[sx, t, rs, :]

    z_early = lax.rem(gx, 2) == 1

    def close_inner(t):
        for part in range(2):
            take_z(2 + part, t)
            with jax.named_scope("P1z"):
                several(*middle[part], 3, close_plane)

    def pre_red(t):
        if t == 0:
            for zd in range(nz):
                msg_sz(zd).wait_recv()
            for m in range(nm):
                sq[m] = jnp.where(low_half, szr[0, m], szr[hi_z, m])
        for m in range(nm):
            own, q = pk[t, m], qb[m + 1]
            zsum = roll(jnp.where(pos0, q, own), 1) + roll(jnp.where(pos3, q, own), -1)
            beside = jnp.where(odd_q, qb[m + 2], qb[m])
            up = jnp.where(bottom, roll(q, 4), q)
            up = jnp.where(no_up, 0.0, pltpu.roll(up, 1, 0))
            down = jnp.where(top, roll(q, -4), q)
            down = jnp.where(no_down, 0.0, pltpu.roll(down, 7, 0))
            rq[m] = (sq[m] + q) + (beside + up) + (down + zsum)

    def open_plane(m):
        for g in inner:
            x0[m + 1, rows_of(g), :] = tile(0, m, g, 0.0)

    def close_plane(m):
        v = eb[m + 1] * jnp.float32(SIXTH)
        for g in inner:
            rs = rows_of(g)
            x0[m + 1, rs, :] = x0[m + 1, rs, :] + jnp.where(ends, edge_at(v, g), 0.0)

    for t in range(SWEEPS):
        final = t == SWEEPS - 1
        with jax.named_scope("P1"):
            several(1, nm - 1, 3, open_plane)
        with jax.named_scope("sent"):
            sent(t)
        for part in range(2):
            take_z(part, t)

        with jax.named_scope("waitxn"):
            for half in range(2):
                take_x(near, half, t)
        with jax.named_scope("P2n"):
            ghost_plane(near, inner)
            red_plane(near * (nm - 1), inner)

        @pl.when(z_early)
        def _():
            close_inner(t)

        for half in range(2):
            groups = (inner[: ng // 2 - 2], inner[ng // 2 - 2 :])[half]
            with jax.named_scope("waitx"):
                take_x(cross, half, t)
            with jax.named_scope("P2"):
                ghost_plane(cross, groups)
                red_plane(cross * (nm - 1), groups)

        @pl.when(jnp.logical_not(z_early))
        def _():
            close_inner(t)

        with jax.named_scope("prered"):
            pre_red(t)

        with jax.named_scope("waity"):
            for sy in range(2):
                if t == 0:
                    msg_sy(sy).wait_recv()
                    for m in range(nm):
                        s0[m + 1, pl.ds((PAD + rows, PAD - 1)[sy], 1), :] = syr[1 - sy, pl.ds(m, 1), :]
                msg_y(sy, t).wait_recv()
                for m in range(nm):
                    x1[m + 1, pl.ds((PAD + rows, PAD - 2)[sy], 2), :] = jr[1 - sy, t, m]
        with jax.named_scope("P3a"):
            for m in range(nm):
                red_plane(m, (0, ng - 1))
        with jax.named_scope("waitfar"):
            for sx in range(2):

                @pl.when(has[sx])
                def _():
                    for sy in range(2):
                        msg_xy(1 - sx, sy, t).wait_recv()
                        x1[(0, nm + 1)[sx], pl.ds((PAD + rows, PAD - 2)[sy], 2), :] = xyr[sx, 1 - sy, t]

            for sy in range(2):
                for zd in range(nz):
                    msg_yz(sy, zd, t).wait_recv()

        with jax.named_scope("P3b"):
            for side in range(2):
                lo, hi = yzr[side, 0, t], yzr[side, hi_z, t]
                yzb[side] = pltpu.roll(jnp.where(lane8 >= cols // 2, lo, hi), (2, (4 * ng - 2) % cols)[side], 1)
                yzb[2 + side] = jnp.where(lane8 == 0, pltpu.roll(lo, 1, 1), pltpu.roll(hi, last, 1))
            for sx in range(2):
                ghost_plane(sx, (0, ng - 1))
            for m in range(nm):
                for g, k in ((-1, 2), (ng, 3)):
                    x0[m + 1, rows_of(g), :] = tile(0, m, g, jnp.broadcast_to(yzb[k, pl.ds(m, 1), :], (8, cols)))
            for m in range(nm):
                total = rq[m] + jnp.where(no_up, jnp.broadcast_to(yzb[0, pl.ds(m, 1), :], (8, cols)), 0.0)
                total = total + jnp.where(no_down, jnp.broadcast_to(yzb[1, pl.ds(m, 1), :], (8, cols)), 0.0)
                rq[m] = total * jnp.float32(SIXTH)
            if final:
                for m in range(nm):
                    er[m] = swapped(rq[m], rq[m])
                break
            for m in range(nm):
                red = rq[m]
                for sy, g in ((0, 0), (1, ng - 1)):
                    y = tile(1, m, g, roll(red, -(4 * g + 1)), None, roll(red, -(4 * g + 3)))
                    put(m, g, y)
                    keep_rows(t + 1, m, y, sy)

        send_far(t + 1)
        with jax.named_scope("P4"):
            for m in range(nm):
                er[m] = swapped(rq[m], rq[m])
            for half, groups in enumerate((inner[: ng // 2 - 1], inner[ng // 2 - 1 :])):
                black_plane(cross * (nm - 1), groups)
                send_x(cross, half, t + 1)
            black_plane(near * (nm - 1), inner)
            for half in range(2):
                send_x(near, half, t + 1)
        pack_edges(t + 1)
        for part in range(2):
            with jax.named_scope("P5"):
                several(*middle[part], 3, lambda m: black_plane(m, inner))
            pack(part, t + 1)


def finish(x0, s1, er, o_hbm, ov, sem):
    planes, rows, cols = ov.shape
    nm, ng, step = planes // 2, rows // 8, 2
    sub = lax.broadcasted_iota(jnp.int32, (8, cols), 0)
    lane = lax.broadcasted_iota(jnp.int32, (8, cols), 1)
    odd = lax.rem(sub + lane, 2) == 1
    first, final_lane = lane == 0, lane == cols - 1

    def out(i):
        at = pl.ds(2 * step * i, 2 * step)
        return pltpu.make_async_copy(ov.at[at], o_hbm.at[at], sem.at[i])

    def plane(m):
        v = er[m]
        for g in range(ng):
            rs = pl.ds(PAD + 8 * g, 8)
            here = x0[m + 1, rs, :]
            beside = jnp.where(odd, x0[m, rs, :], x0[m + 2, rs, :])
            edge = pltpu.roll(v, (2 * cols - (4 * g + 2)) % cols, 1)
            total = (s1[m, rs, :] + here) + (beside + x0[m + 1, pl.ds(PAD + 8 * g - 1, 8), :])
            total = total + x0[m + 1, pl.ds(PAD + 8 * g + 1, 8), :]
            total = total + jnp.where(first, edge, pltpu.roll(here, 1, 1))
            total = total + jnp.where(final_lane, edge, pltpu.roll(here, cols - 1, 1))
            y = total * jnp.float32(SIXTH)
            to = pl.ds(8 * g, 8)
            ov[2 * m, to, :] = jnp.where(odd, y, here)
            ov[2 * m + 1, to, :] = jnp.where(odd, here, y)

    def body(i, carry):
        for k in range(step):
            plane(step * i + k)

        @pl.when(i > 0)
        def _():
            out(i - 1).start()

        return carry

    lax.fori_loop(0, nm // step, body, 0)
    out(nm // step - 1).start()
    for i in range(nm // step):
        out(i).wait()


def solution(mesh):
    sizes = tuple(mesh.shape[a] for a in ("gx", "gy", "gz"))

    def on_device(field, source):
        planes, rows, cols = field.shape
        nm, ng, nz = planes // 2, rows // 8, 1 if sizes[2] == 2 else 2
        assert planes % 4 == 0 and nm >= 4 and rows % 8 == 0 and cols == 128 and 4 * ng <= cols
        _, rounds, total_slots = slots(nz)
        f32 = jnp.float32
        vm = lambda *shape: pltpu.VMEM(shape, f32)
        shape = lambda *dims: jax.ShapeDtypeStruct(dims, f32)
        in_vmem = pl.BlockSpec(memory_space=pltpu.VMEM)
        wide = rows + 2 * PAD
        kept = pl.pallas_call(
            functools.partial(kernel, sizes),
            out_shape=[shape(nm + 2, wide, cols), shape(nm, wide, cols), shape(nm, 8, cols)],
            in_specs=[pl.BlockSpec(memory_space=pltpu.HBM)] * 2,
            out_specs=[in_vmem] * 3,
            scratch_shapes=[
                vm(*field.shape),
                vm(*field.shape),
                vm(nm + 2, wide, cols),
                vm(nm + 2, wide, cols),
                vm(nm + 2, 8, cols),
                vm(nm, 8, cols),
                vm(nm + 2, 8, cols),
                vm(nm, 8, cols),
                vm(4, nm, cols),
                vm(nm, 8, cols),
                vm(SWEEPS, nm, 8, cols),
                vm(2, SWEEPS, nm, 2, cols),
                vm(2, SWEEPS, nm, cols),
                vm(2, nm, cols),
                vm(2, rows // 2, cols),
                vm(2, rows // 2, cols),
                vm(2, SWEEPS, rows, cols),
                vm(2, SWEEPS, nm, 2, cols),
                vm(nz, SWEEPS, nm, 8, cols),
                vm(2, 2, SWEEPS, 2, cols),
                vm(2, nz, SWEEPS, nm, cols),
                vm(2, nz, SWEEPS, 8, cols),
                vm(2, nm, cols),
                vm(nz, nm, 8, cols),
                pltpu.SemaphoreType.DMA((total_slots,)),
                pltpu.SemaphoreType.DMA((total_slots + rounds,)),
                pltpu.SemaphoreType.DMA((6,)),
                pltpu.SemaphoreType.DMA((4,)),
            ],
            compiler_params=pltpu.CompilerParams(
                collective_id=0, has_side_effects=True, vmem_limit_bytes=51 * 1024 * 1024
            ),
        )(field, source)
        return pl.pallas_call(
            finish,
            out_shape=shape(planes, rows, cols),
            in_specs=[in_vmem] * 3,
            out_specs=pl.BlockSpec(memory_space=pltpu.HBM),
            scratch_shapes=[vm(planes, rows, cols), pltpu.SemaphoreType.DMA((nm // 2,))],
            compiler_params=pltpu.CompilerParams(vmem_limit_bytes=12 * 1024 * 1024),
        )(*kept)

    spec = P("gx", "gy", "gz")
    return jax.shard_map(on_device, mesh=mesh, in_specs=(spec, spec), out_specs=spec, check_vma=False)
```
